512 devices in a mesh: groups: 2 (over y), expert: 32 (over z, core), dp: 8 (over x).
Axes of the slice: x: 8, y: 2, z: 16, core: 2. Of those that a mesh axis runs over, the one named last changes fastest.
The devices are a block of a 8x16x16 slice.
Arguments:
- tokens: bfloat16 [4096, 2048], P(('groups', 'expert'), 'dp'), parts along dimension 0, may hold values from -6 to 6
- expert_ids: int32 [4096, 8], P(('groups', 'expert')), parts along dimension 0, may hold values from 0 to 63, all different within a row; in each aligned block of 64 rows (0 to 63, 64 to 127, ...) at most 16 rows name the same one
- gate_levels: int32 [4096, 8], P(('groups', 'expert')), parts along dimension 0, may hold values from 1 to 255
- gate_weight: bfloat16 [64, 2048, 1536], P('expert', None, 'dp'), may hold values from -0.125 to 0.125
- up_weight: bfloat16 [64, 2048, 1536], P('expert', None, 'dp'), may hold values from -0.125 to 0.125
- down_weight: bfloat16 [64, 1536, 2048], P('expert', None, 'dp'), may hold values from -0.15625 to 0.15625
Outputs:
- mixed: bfloat16 [4096, 2048], P(('groups', 'expert'), 'dp'), parts along dimension 0
The draws below stay inside these ranges and needn't reach their ends.
There are 2 independent parts, one for each index of `groups`. The reference program is written for one: setup_inputs(seed, part) draws one part's arguments, and reference() takes and returns one part's arrays. A program takes and returns all parts, laid end to end along the dimension named above; an argument that names none is the same for every part. Nothing has to cross between parts.
Inputs may be any that keep to these rules, and one draw needn't show every extreme that they name: `expert_ids`: each row names 8 different experts. Among the rows of one index of the expert axis no expert is named more than 16 times, a bound that some block reaches.
All inputs are finite; a program needn't handle non-finite values.
Results may differ from the reference program's by a relative error of at most 0.0057.
Values may be sent and summed in bfloat16 or wider, within the bound.
No kernel may reach another device: no remote copies, remote signals or barrier semaphores. Data moves between devices by JAX's collectives and lax.ppermute only.
A program may use at most 64 MiB of HBM per device.

```python
import math
import jax
import jax.numpy as jnp
import numpy as np
from jax import lax

D = 2048
FF = 1536
TOP = 8
TOK_DEV = 64
EXPERTS = 64
TOKENS = 2048
CAP = 16
N_EXPERT = 32


def with_ends(drawn, key, least, top_value):
    longest = drawn.shape.index(max(drawn.shape))
    spots = []
    for shift in (0, 1):
        where = [jax.random.randint(jax.random.fold_in(key, axis), (), 0, length) for axis, length in enumerate(drawn.shape)]
        where[longest] = (where[longest] + shift) % drawn.shape[longest]
        spots.append(tuple(where))
    return drawn.at[spots[0]].set(least).at[spots[1]].set(top_value)


def level_of(own_key, dims, split, least, largest):
    def one(dim, blocks):
        steps = jax.random.uniform(jax.random.fold_in(jax.random.fold_in(own_key, 6), dim), (blocks,), jnp.float32, least / len(split), largest / len(split))
        return jnp.repeat(jnp.exp(steps), dims[dim] // blocks).reshape((-1,) + (1,) * (len(dims) - dim - 1))

    level = one(*split[0])
    for cut in split[1:]:
        level = level * one(*cut)
    return level


def routed_block(key, own, number, rows, number_of, top, bound, skew):
    ranking = jax.random.permutation(key, number_of)
    packed, usual = load_shares(number_of, rows * top, bound, skew, True), load_shares(number_of, rows * top, bound, skew, False)
    places = jnp.arange(number_of)

    def named(lengths, turn):
        used = int((lengths > 0).sum())
        fixed = max(1, used // 4)
        shifted = fixed + (places - fixed + turn * (used - fixed)) % max(1, number_of - fixed)
        return jnp.zeros((number_of,), jnp.int32).at[ranking[jnp.where(places < fixed, places, shifted)]].set(jnp.asarray(lengths, jnp.int32))

    lengths = jnp.where(number % 4 == 0, named(packed, number // 4), named(usual, number - number // 4 - 1))
    mixed = jax.random.permutation(jax.random.fold_in(own, 3), number_of)
    donor, sink = mixed[0:number_of // 2 * 2:2], mixed[1:number_of // 2 * 2:2]
    slack = jnp.minimum(lengths[donor] - 1, bound - lengths[sink]) // 2
    slack = jnp.where((donor == ranking[0]) | (sink == ranking[0]) | (lengths[sink] == 0), 0, jnp.maximum(slack, 0))
    shifted = jax.random.randint(jax.random.fold_in(own, 4), (number_of // 2,), 0, 1 << 20) % (slack + 1)
    lengths = lengths.at[donor].add(-shifted).at[sink].add(shifted)
    members = jnp.searchsorted(jnp.cumsum(lengths), jnp.arange(rows * top), side="right").astype(jnp.int32)
    grid = members.reshape(top, rows).T
    grid = grid[jax.random.permutation(jax.random.fold_in(own, 1), rows)]
    turn = jax.random.randint(jax.random.fold_in(own, 2), (rows, 1), 0, top)
    return jnp.take_along_axis(grid, (jnp.arange(top)[None, :] + turn) % top, axis=1)


def load_shares(amount, total, most, lean, full):
    weights = [(1 << 20) // math.isqrt(grade ** lean) + 1 for grade in range(1, amount + 1)]
    largest = most if full else min(most, max(-(-total // amount), total * weights[0] // sum(weights)))
    least = 1 if total - largest >= amount - 1 else 0
    given, rest = [largest] + [least] * (amount - 1), total - largest - least * (amount - 1)
    while rest > 0:
        candidates = [i for i in range(1, amount) if given[i] < largest] or [i for i in range(1, amount) if given[i] < most]
        mass, budget = sum([weights[i] for i in candidates]), rest
        for i in candidates:
            extra = min(most - given[i], max(1, budget * weights[i] // mass), rest)
            given[i] = given[i] + extra
            rest = rest - extra
    return np.array(given)


def bell_draw(key, shape, scale, reach, split=(), kind=jnp.bfloat16):
    array = jax.random.normal(key, shape, jnp.float32) * scale
    if len(split) > 0:
        array = level_of(key, shape, split, -0.22, 0.18) * array
    return jnp.clip(array, min=-reach, max=reach).astype(kind)


def setup_inputs(seed: int = 0, part: int = 0) -> dict:
    arg_keys = jax.random.split(jax.random.key(seed), 7)
    own_keys = jax.random.split(jax.random.fold_in(arg_keys[6], part), 7)
    tokens = bell_draw(own_keys[0], (TOKENS, D), 1.0, 6.0, ((0, 32), (1, 8)))
    expert_ids_keys = jax.random.split(jax.random.fold_in(own_keys[1], 1), TOKENS // TOK_DEV)
    expert_ids_turns = jax.random.permutation(jax.random.fold_in(own_keys[1], 3), TOKENS // TOK_DEV)
    expert_ids = jax.vmap(lambda own, number: routed_block(jax.random.fold_in(own_keys[1], 2), own, number, TOK_DEV, EXPERTS, TOP, CAP, 2))(expert_ids_keys, expert_ids_turns).reshape((TOKENS, TOP))
    gate_levels = with_ends(jax.random.randint(own_keys[2], (TOKENS, TOP), 1, 256), jax.random.fold_in(own_keys[2], 1), 1, 255).astype(jnp.int32)
    gate_weight = bell_draw(arg_keys[3], (EXPERTS, D, FF), D ** -0.5, 0.125, ((0, 32), (2, 8)))
    up_weight = bell_draw(arg_keys[4], (EXPERTS, D, FF), D ** -0.5, 0.125, ((0, 32), (2, 8)))
    down_weight = bell_draw(arg_keys[5], (EXPERTS, FF, D), FF ** -0.5, 0.15625, ((0, 32), (2, 8)))
    return dict(tokens=tokens, expert_ids=expert_ids, gate_levels=gate_levels, gate_weight=gate_weight, up_weight=up_weight, down_weight=down_weight)


def reference(tokens, expert_ids, gate_levels, gate_weight, up_weight, down_weight):
    shares = gate_levels.astype(jnp.float32) / 256.0
    row_limit = N_EXPERT * CAP
    count_tokens = tokens.shape[0]

    def per_expert(running, expert_index):
        matched = expert_ids == expert_index
        weight_sum = jnp.sum(jnp.where(matched, shares, jnp.float32(0.0)), axis=1)
        chosen = jnp.any(matched, axis=1)
        token_rows = jnp.nonzero(chosen, size=row_limit, fill_value=0)[0].astype(jnp.int32)
        picked = tokens[token_rows]
        gate_part = jnp.dot(picked, gate_weight[expert_index], preferred_element_type=jnp.float32)
        up_part = jnp.dot(picked, up_weight[expert_index], preferred_element_type=jnp.float32)
        hidden = (jax.nn.silu(gate_part) * up_part).astype(jnp.bfloat16)
        expert_out = jnp.dot(hidden, down_weight[expert_index], preferred_element_type=jnp.float32).astype(jnp.bfloat16)
        filled = jnp.arange(row_limit, dtype=jnp.int32) < jnp.sum(chosen.astype(jnp.int32))
        factor = jnp.where(filled, weight_sum[token_rows], jnp.float32(0.0))
        running = running.at[token_rows].add(factor[:, None] * expert_out.astype(jnp.float32))
        return running, None

    start_sum = jnp.zeros((count_tokens, tokens.shape[1]), jnp.float32)
    labels = jnp.arange(gate_weight.shape[0], dtype=jnp.int32)
    total_sum, unused = lax.scan(per_expert, start_sum, labels)
    return total_sum.astype(jnp.bfloat16)
```

```python
import jax
import jax.numpy as jnp
from jax import lax
from jax.sharding import Mesh, PartitionSpec as P

CORES = 2


def shift(block, axis, step):
    count = lax.axis_size(axis)
    return lax.ppermute(block, axis, [(i, (i + step) % count) for i in range(count)])


def ring_feed(block, axis, consume):
    count = lax.axis_size(axis)
    me = lax.axis_index(axis)
    half = count // 2
    right = left = block
    consume(block, me, None)
    for step in range(1, half):
        right = shift(right, axis, 1)
        left = shift(left, axis, -1)
        consume(right, (me - step) % count, None)
        consume(left, (me + step) % count, None)
    middle = block.shape[0] // 2
    right = shift(right[:middle], axis, 1)
    left = shift(left[middle:], axis, -1)
    consume(right, (me + half) % count, (0, middle))
    consume(left, (me + half) % count, (middle, block.shape[0]))


def positions(member):
    count = member.shape[-1]
    row = lax.broadcasted_iota(jnp.int32, (count, count), 0)
    col = lax.broadcasted_iota(jnp.int32, (count, count), 1)
    before = (row < col).astype(jnp.bfloat16)
    return jnp.einsum(
        "...i,ij->...j", member.astype(jnp.bfloat16), before, preferred_element_type=jnp.float32
    ).astype(jnp.int32)


def on_device(tokens, expert_ids, gate_levels, gate_weight, up_weight, down_weight):
    tok_dev, width = tokens.shape
    picks = expert_ids.shape[1]
    exp_dev = gate_weight.shape[0]
    hid = gate_weight.shape[2]
    out_features = down_weight.shape[2]
    n_z = lax.axis_size("z")
    chip_experts = exp_dev * CORES
    experts = chip_experts * n_z
    capacity = min(tok_dev, max(2, 2 * tok_dev * picks // experts))
    core = lax.axis_index("core")
    z = lax.axis_index("z")

    swap = [(0, 1), (1, 0)]
    weight_in = jnp.concatenate([gate_weight, up_weight], axis=2)
    weight_in = jnp.concatenate([weight_in, lax.ppermute(weight_in, "core", swap)], axis=0)
    weight_out = jnp.concatenate([down_weight, lax.ppermute(down_weight, "core", swap)], axis=0)

    ids_rows = jnp.zeros((2 * picks, width), jnp.bfloat16)
    ids_rows = ids_rows.at[:picks, :tok_dev].set(expert_ids.T.astype(jnp.bfloat16))
    gathered = lax.all_gather(jnp.concatenate([tokens, ids_rows], axis=0), "z", axis=0)
    all_tokens = gathered[:, :tok_dev]
    all_ids = gathered[:, tok_dev : tok_dev + picks, :tok_dev].astype(jnp.int32)

    local = jnp.arange(chip_experts, dtype=jnp.int32)
    owner_core = jnp.where(local < exp_dev, core, 1 - core)
    names = (z * CORES + owner_core) * exp_dev + local % exp_dev
    member = jnp.any(all_ids[:, None, :, :] == names[None, :, None, None], axis=2)
    spot = jnp.where(member, positions(member), -1)
    chosen = spot[:, :, None, :] == jnp.arange(capacity, dtype=jnp.int32)[None, None, :, None]
    rows = jnp.einsum(
        "sepj,sjd->espd",
        chosen.astype(jnp.bfloat16),
        all_tokens,
        preferred_element_type=jnp.float32,
    ).astype(jnp.bfloat16)
    count = n_z * capacity
    rows = rows.reshape(chip_experts, count, width)

    total = [jnp.zeros((chip_experts, count, 2 * hid), jnp.float32)]

    def feed_in(part, owner, span):
        low, high = span or (0, chip_experts)
        weights = lax.dynamic_slice(
            weight_in[low:high], (0, owner * width, 0), (high - low, width, 2 * hid)
        )
        term = jnp.einsum("xcd,xdf->xcf", part, weights, preferred_element_type=jnp.float32)
        total[0] = total[0] + term if span is None else total[0].at[low:high].add(term)

    ring_feed(rows, "dp", feed_in)
    gate_next, up_next = total[0][..., :hid], total[0][..., hid:]
    hidden = (jax.nn.silu(gate_next) * up_next).astype(jnp.bfloat16)

    outputs = [jnp.zeros((chip_experts, count, out_features), jnp.float32)]

    def feed_out(part, owner, span):
        low, high = span or (0, chip_experts)
        weights = lax.dynamic_slice(
            weight_out[low:high], (0, owner * hid, 0), (high - low, hid, out_features)
        )
        term = jnp.einsum("xcf,xfk->xck", part, weights, preferred_element_type=jnp.float32)
        outputs[0] = outputs[0] + term if span is None else outputs[0].at[low:high].add(term)

    ring_feed(hidden, "dp", feed_out)
    result = outputs[0].astype(jnp.bfloat16).reshape(chip_experts, n_z, capacity, out_features)
    result = jnp.transpose(result, (1, 0, 2, 3))
    returned = lax.all_to_all(result, "z", split_axis=0, concat_axis=0, tiled=True)
    slot_count = experts * capacity
    returned = returned.reshape(slot_count, out_features)

    own_ids = expert_ids.T
    every = jnp.arange(experts, dtype=jnp.int32)
    in_chip = every % chip_experts
    turned = (in_chip + core * exp_dev) % chip_experts
    names = every - in_chip + turned
    named = own_ids[None, :, :] == names[:, None, None]
    own_spot = positions(jnp.any(named, axis=1))
    shares = gate_levels.astype(jnp.float32) / 256.0
    factor = jnp.sum(jnp.where(named, shares.T[None, :, :], 0.0), axis=1)
    weighting = jnp.where(
        own_spot[:, None, :] == jnp.arange(capacity, dtype=jnp.int32)[None, :, None],
        factor[:, None, :],
        0.0,
    ).astype(jnp.bfloat16)
    weighting = weighting.reshape(slot_count, tok_dev)
    combined = jnp.einsum("sj,sd->jd", weighting, returned, preferred_element_type=jnp.float32)
    return combined.astype(jnp.bfloat16)


def solution(mesh):
    groups, expert, dp = (mesh.shape[name] for name in ("groups", "expert", "dp"))
    split = Mesh(
        mesh.devices.reshape(groups, expert // CORES, CORES, dp), ("groups", "z", "core", "dp")
    )
    rows, held = ("groups", "z", "core"), ("z", "core")
    in_specs = (
        P(rows, "dp"),
        P(rows, None),
        P(rows, None),
        P(held, None, "dp"),
        P(held, None, "dp"),
        P(held, None, "dp"),
    )
    return jax.shard_map(
        on_device, mesh=split, in_specs=in_specs, out_specs=P(rows, "dp"), check_vma=False
    )
```

```python
import jax
import jax.numpy as jnp
from jax import lax
from jax.sharding import Mesh, PartitionSpec as P

CORES = 2


def swap(block):
    return lax.ppermute(block, "core", [(0, 1), (1, 0)])


def shift(block, step):
    count = lax.axis_size("dp")
    return lax.ppermute(block, "dp", [(i, (i + step) % count) for i in range(count)])


def positions(member):
    count = member.shape[-1]
    row = lax.broadcasted_iota(jnp.int32, (count, count), 0)
    col = lax.broadcasted_iota(jnp.int32, (count, count), 1)
    before = (row < col).astype(jnp.bfloat16)
    return jnp.einsum(
        "...i,ij->...j", member.astype(jnp.bfloat16), before, preferred_element_type=jnp.float32
    ).astype(jnp.int32)


def ring_sum(own, term):
    count = lax.axis_size("dp")
    half = count // 2
    me = lax.axis_index("dp")
    total = term(own, me)
    up = down = own
    for step in range(1, half):
        with jax.named_scope(f"up_{step}"):
            up = shift(up, 1)
        with jax.named_scope(f"down_{step}"):
            down = shift(down, -1)
        total = total + term(up, (me - step) % count)
        total = total + term(down, (me + step) % count)
    middle = own.shape[0] // 2
    with jax.named_scope("up_last"):
        up = shift(up[:middle], 1)
    with jax.named_scope("down_last"):
        down = shift(down[middle:], -1)
    return total + term(jnp.concatenate([up, down], axis=0), (me + half) % count)


def on_device(tokens, expert_ids, gate_levels, gate_weight, up_weight, down_weight):
    tok_dev, width = tokens.shape
    picks = expert_ids.shape[1]
    exp_dev = gate_weight.shape[0]
    hid = gate_weight.shape[2]
    n_z = lax.axis_size("z")
    chip_experts = exp_dev * CORES
    experts = chip_experts * n_z
    capacity = min(tok_dev, max(2, 2 * tok_dev * picks // experts))
    core = lax.axis_index("core")
    z = lax.axis_index("z")

    ids_rows = jnp.zeros((2 * picks, width), jnp.bfloat16)
    ids_rows = ids_rows.at[:picks, :tok_dev].set(expert_ids.T.astype(jnp.bfloat16))
    gathered = lax.all_gather(jnp.concatenate([tokens, ids_rows], axis=0), "z", axis=0)
    all_tokens = gathered[:, :tok_dev]
    all_ids = gathered[:, tok_dev : tok_dev + picks, :tok_dev].astype(jnp.int32)

    local = jnp.arange(chip_experts, dtype=jnp.int32)
    owner_core = jnp.where(local < exp_dev, core, 1 - core)
    names = (z * CORES + owner_core) * exp_dev + local % exp_dev
    member = jnp.any(all_ids[:, None, :, :] == names[None, :, None, None], axis=2)
    spot = jnp.where(member, positions(member), -1)
    chosen = spot[:, :, None, :] == jnp.arange(capacity, dtype=jnp.int32)[None, None, :, None]
    rows = jnp.einsum(
        "sepj,sjd->espd",
        chosen.astype(jnp.bfloat16),
        all_tokens,
        preferred_element_type=jnp.float32,
    ).astype(jnp.bfloat16)
    count = n_z * capacity
    rows = rows.reshape(chip_experts, count, width)

    with jax.named_scope("weights_in"):
        weight_in = [jnp.swapaxes(w, 1, 2) for w in (gate_weight, up_weight)]
        weight_in = jnp.concatenate(
            [jnp.concatenate(weight_in, axis=1), jnp.concatenate([swap(w) for w in weight_in], axis=1)],
            axis=0,
        )
    with jax.named_scope("weights_out"):
        weight_out = jnp.concatenate([down_weight, swap(down_weight)], axis=0)

    def term_in(part, owner):
        weights = lax.dynamic_slice_in_dim(weight_in, owner * width, width, 2)
        return jnp.einsum("xfd,xcd->xfc", weights, part, preferred_element_type=jnp.float32)

    with jax.named_scope("tokens_round"):
        mixed = ring_sum(rows, term_in)
    gate_next, up_next = mixed[:, :hid], mixed[:, hid:]
    hidden = (jax.nn.silu(gate_next) * up_next).astype(jnp.bfloat16)

    def term_out(part, owner):
        weights = lax.dynamic_slice_in_dim(weight_out, owner * hid, hid, 1)
        return jnp.einsum("xfc,xfk->xck", part, weights, preferred_element_type=jnp.float32)

    with jax.named_scope("hidden_round"):
        result = ring_sum(hidden, term_out).astype(jnp.bfloat16)
    out_features = result.shape[2]
    result = result.reshape(chip_experts, n_z, capacity, out_features)
    result = jnp.transpose(result, (1, 0, 2, 3))
    returned = lax.all_to_all(result, "z", split_axis=0, concat_axis=0, tiled=True)
    slot_count = experts * capacity
    returned = returned.reshape(slot_count, out_features)

    own_ids = expert_ids.T
    every = jnp.arange(experts, dtype=jnp.int32)
    in_chip = every % chip_experts
    turned = (in_chip + core * exp_dev) % chip_experts
    names = every - in_chip + turned
    named = own_ids[None, :, :] == names[:, None, None]
    own_spot = positions(jnp.any(named, axis=1))
    shares = gate_levels.astype(jnp.float32) / 256.0
    factor = jnp.sum(jnp.where(named, shares.T[None, :, :], 0.0), axis=1)
    weighting = jnp.where(
        own_spot[:, None, :] == jnp.arange(capacity, dtype=jnp.int32)[None, :, None],
        factor[:, None, :],
        0.0,
    ).astype(jnp.bfloat16)
    weighting = weighting.reshape(slot_count, tok_dev)
    combined = jnp.einsum("sj,sd->jd", weighting, returned, preferred_element_type=jnp.float32)
    return combined.astype(jnp.bfloat16)


def solution(mesh):
    groups, expert, dp = (mesh.shape[name] for name in ("groups", "expert", "dp"))
    split = Mesh(
        mesh.devices.reshape(groups, expert // CORES, CORES, dp), ("groups", "z", "core", "dp")
    )
    rows, held = ("groups", "z", "core"), ("z", "core")
    in_specs = (
        P(rows, "dp"),
        P(rows, None),
        P(rows, None),
        P(held, None, "dp"),
        P(held, None, "dp"),
        P(held, None, "dp"),
    )
    return jax.shard_map(
        on_device, mesh=split, in_specs=in_specs, out_specs=P(rows, "dp"), check_vma=False
    )
```

```python
import jax
import jax.numpy as jnp
from jax import lax
from jax.experimental import pallas as pl
from jax.experimental.pallas import tpu as pltpu
from jax.sharding import Mesh, PartitionSpec as P


CORES = 2


def swap(block):
    return lax.ppermute(block, "core", [(0, 1), (1, 0)])


def onward(block):
    count = lax.axis_size("dp")
    up = [(i, (i + 1) % count) for i in range(count)]
    down = [(count + i, count + (i - 1) % count) for i in range(count)]
    return lax.ppermute(block, ("core", "dp"), up + down)


def positions(member):
    count = member.shape[-1]
    row = lax.broadcasted_iota(jnp.int32, (count, count), 0)
    col = lax.broadcasted_iota(jnp.int32, (count, count), 1)
    before = (row < col).astype(jnp.bfloat16)
    return jnp.einsum(
        "...i,ij->...j", member.astype(jnp.bfloat16), before, preferred_element_type=jnp.float32
    ).astype(jnp.int32)


def weighted_sum(parts, steps, weights, table, kind, extra=(), finish=None, out=None):
    chip_experts = parts[0].shape[0]
    hid, rows = None, None
    exp_dev = weights[0][0].shape[0]
    last = table.shape[0] - 1
    n_parts, n_kinds = len(parts), len(weights)

    def place(core):
        return lambda e, t: jnp.clip(e - exp_dev * core(t), 0, exp_dev - 1)

    ours = place(lambda t: t[last])
    theirs = place(lambda t: 1 - t[last])
    if kind == "in":
        hid, width = weights[0][0].shape[1], parts[0].shape[2]
        block = (1, hid, width)
        where = lambda pick, k: lambda e, t: (pick(e, t), 0, t[k])
        rows = parts[0].shape[1]
        sum_shape = (n_kinds * hid, rows)
        dims = (((1,), (1,)), ((), ()))
    else:
        hid, width = parts[0].shape[1], weights[0][0].shape[2]
        block = (1, hid, width)
        where = lambda pick, k: lambda e, t: (pick(e, t), t[k], 0)
        rows = parts[0].shape[2]
        sum_shape = (rows, width)
        dims = (((0,), (0,)), ((), ()))

    in_specs = [pl.BlockSpec((1, *p.shape[1:]), lambda e, t: (e, 0, 0)) for p in parts]
    operands = list(parts)
    for k in steps:
        for first, second in weights:
            in_specs += [pl.BlockSpec(block, where(ours, k)), pl.BlockSpec(block, where(theirs, k))]
            operands += [first, second]
    for more in extra:
        in_specs.append(pl.BlockSpec((1, *sum_shape), lambda e, t: (e, 0, 0)))
        operands.append(more)
    if out is None:
        out_shape = jax.ShapeDtypeStruct((chip_experts, *sum_shape), jnp.float32)
        out_spec = pl.BlockSpec((1, *sum_shape), lambda e, t: (e, 0, 0))
    else:
        out_shape, out_spec = out

    def body(table_ref, *refs):
        part_refs, rest = refs[:n_parts], refs[n_parts:]
        weight_refs, rest = rest[: 2 * n_parts * n_kinds], rest[2 * n_parts * n_kinds :]
        extra_refs, out_ref = rest[:-1], rest[-1]
        mine = pl.program_id(0) // exp_dev == table_ref[last]
        sums = []
        for kind_at in range(n_kinds):
            total = None
            for k in range(n_parts):
                at = 2 * (k * n_kinds + kind_at)
                weight = jnp.where(mine, weight_refs[at][0], weight_refs[at + 1][0])
                pair = (weight, part_refs[k][0]) if kind == "in" else (part_refs[k][0], weight)
                term = lax.dot_general(*pair, dims, preferred_element_type=jnp.float32)
                total = term if total is None else total + term
            if kind == "in":
                for ref in extra_refs:
                    total = total + ref[0, kind_at * hid : (kind_at + 1) * hid]
            else:
                for ref in extra_refs:
                    total = total + ref[0]
            sums.append(total)
        if finish is not None:
            finish(out_ref, *sums)
        elif kind == "in":
            for kind_at, total in enumerate(sums):
                out_ref[0, kind_at * hid : (kind_at + 1) * hid] = total
        else:
            out_ref[0] = sums[0]

    flops = 2 * chip_experts * n_parts * n_kinds * rows * hid * width
    moved = n_parts * chip_experts * (n_kinds * hid * width + parts[0].size // chip_experts) * 2
    return pl.pallas_call(
        body,
        grid_spec=pltpu.PrefetchScalarGridSpec(
            num_scalar_prefetch=1, grid=(chip_experts,), in_specs=in_specs, out_specs=out_spec
        ),
        out_shape=out_shape,
        compiler_params=pltpu.CompilerParams(vmem_limit_bytes=16 * 2**20),
        cost_estimate=pl.CostEstimate(flops=flops, bytes_accessed=moved, transcendentals=0),
    )(table, *operands)


def gather_sum(own, weights, table, kind, finish, out):
    half = lax.axis_size("dp") // 2
    mine = [own]
    for _ in range(1, half + 1):
        mine.append(onward(mine[-1]))
    other = [swap(own)]
    for _ in range(1, half):
        other.append(onward(other[-1]))
    early = weighted_sum(mine[:half], range(half), weights, table, kind)
    aside = weighted_sum(other[1:], range(1, half), weights, table, kind)
    back = swap(aside)
    return weighted_sum(mine[half:], [half], weights, table, kind, (early, back), finish, out)


def layer(tokens, expert_ids, gate_levels, gate_weight, up_weight, down_weight):
    tok_dev, width = tokens.shape
    picks = expert_ids.shape[1]
    exp_dev = gate_weight.shape[0]
    hid = gate_weight.shape[2]
    n_z = lax.axis_size("z")
    chip_experts = exp_dev * CORES
    experts = chip_experts * n_z
    capacity = min(tok_dev, max(2, 2 * tok_dev * picks // experts))
    core = lax.axis_index("core")
    z = lax.axis_index("z")

    ids_rows = jnp.zeros((2 * picks, width), jnp.bfloat16)
    ids_rows = ids_rows.at[:picks, :tok_dev].set(expert_ids.T.astype(jnp.bfloat16))
    gathered = lax.all_gather(jnp.concatenate([tokens, ids_rows], axis=0), "z", axis=0)
    all_tokens = gathered[:, :tok_dev]
    all_ids = gathered[:, tok_dev : tok_dev + picks, :tok_dev].astype(jnp.int32)

    names = z * chip_experts + jnp.arange(chip_experts, dtype=jnp.int32)
    member = jnp.any(all_ids[:, None, :, :] == names[None, :, None, None], axis=2)
    spot = jnp.where(member, positions(member), -1)
    chosen = spot[:, :, None, :] == jnp.arange(capacity, dtype=jnp.int32)[None, None, :, None]
    rows = jnp.einsum(
        "sepj,sjd->espd",
        chosen.astype(jnp.bfloat16),
        all_tokens,
        preferred_element_type=jnp.float32,
    ).astype(jnp.bfloat16)
    count = n_z * capacity
    rows = rows.reshape(chip_experts, count, width)

    pairs = []
    for weights in (jnp.swapaxes(gate_weight, 1, 2), jnp.swapaxes(up_weight, 1, 2), down_weight):
        pairs.append((weights, swap(weights)))

    n_dp = lax.axis_size("dp")
    step = jnp.arange(n_dp, dtype=jnp.int32)
    owners = (lax.axis_index("dp") + jnp.where(core == 0, -step, step)) % n_dp
    table = jnp.where(step == n_dp - 1, core, owners)

    def gated(out_ref, gate_sum, up_sum):
        out_ref[0] = (gate_sum / (1.0 + jnp.exp(-gate_sum)) * up_sum).astype(jnp.bfloat16)

    hidden = gather_sum(
        rows,
        pairs[:2],
        table,
        "in",
        gated,
        (
            jax.ShapeDtypeStruct((chip_experts, hid, count), jnp.bfloat16),
            pl.BlockSpec((1, hid, count), lambda e, t: (e, 0, 0)),
        ),
    )

    out_features = down_weight.shape[2]

    def returning(out_ref, total):
        out_ref[:, 0] = total.astype(jnp.bfloat16).reshape(n_z, capacity, out_features)

    result = gather_sum(
        hidden,
        pairs[2:],
        table,
        "out",
        returning,
        (
            jax.ShapeDtypeStruct((n_z, chip_experts, capacity, out_features), jnp.bfloat16),
            pl.BlockSpec((n_z, 1, capacity, out_features), lambda e, t: (0, e, 0, 0)),
        ),
    )
    returned = lax.all_to_all(result, "z", split_axis=0, concat_axis=0, tiled=True)
    slot_count = experts * capacity
    returned = returned.reshape(slot_count, out_features)

    own_ids = expert_ids.T
    names = jnp.arange(experts, dtype=jnp.int32)
    named = own_ids[None, :, :] == names[:, None, None]
    own_spot = positions(jnp.any(named, axis=1))
    shares = gate_levels.astype(jnp.float32) / 256.0
    factor = jnp.sum(jnp.where(named, shares.T[None, :, :], 0.0), axis=1)
    weighting = jnp.where(
        own_spot[:, None, :] == jnp.arange(capacity, dtype=jnp.int32)[None, :, None],
        factor[:, None, :],
        0.0,
    ).astype(jnp.bfloat16)
    weighting = weighting.reshape(slot_count, tok_dev)
    combined = jnp.einsum("sj,sd->jd", weighting, returned, preferred_element_type=jnp.float32)
    return combined.astype(jnp.bfloat16)


def solution(mesh):
    groups, expert, dp = (mesh.shape[name] for name in ("groups", "expert", "dp"))
    split = Mesh(
        mesh.devices.reshape(groups, expert // CORES, CORES, dp), ("groups", "z", "core", "dp")
    )
    rows, held = ("groups", "z", "core"), ("z", "core")
    in_specs = (
        P(rows, "dp"),
        P(rows, None),
        P(rows, None),
        P(held, None, "dp"),
        P(held, None, "dp"),
        P(held, None, "dp"),
    )
    return jax.shard_map(
        layer, mesh=split, in_specs=in_specs, out_specs=P(rows, "dp"), check_vma=False
    )
```

```python
import jax
import jax.numpy as jnp
from jax import lax
from jax.experimental import pallas as pl
from jax.experimental.pallas import tpu as pltpu
from jax.sharding import Mesh, PartitionSpec as P


CORES = 2


def swap(block):
    return lax.ppermute(block, "core", [(0, 1), (1, 0)])


def onward(block):
    count = lax.axis_size("dp")
    up = [(i, (i + 1) % count) for i in range(count)]
    down = [(count + i, count + (i - 1) % count) for i in range(count)]
    return lax.ppermute(block, ("core", "dp"), up + down)


def positions(member):
    count = member.shape[-1]
    row = lax.broadcasted_iota(jnp.int32, (count, count), 0)
    col = lax.broadcasted_iota(jnp.int32, (count, count), 1)
    before = (row < col).astype(jnp.bfloat16)
    return jnp.einsum(
        "...i,ij->...j", member.astype(jnp.bfloat16), before, preferred_element_type=jnp.float32
    ).astype(jnp.int32)


def weighted_sum(parts, steps, weights, table, kind, ours_first, extra=(), finish=None, out=None):
    chip_experts = parts[0].shape[0]
    exp_dev = weights[0][0].shape[0]
    n_parts, n_kinds = len(parts), len(weights)
    into = kind == "in"
    if into:
        hid, width = weights[0][0].shape[1], parts[0].shape[2]
        rows = parts[0].shape[1]
        sum_shape = (n_kinds * hid, rows)
        dims = (((1,), (1,)), ((), ()))
    else:
        hid, width = parts[0].shape[1], weights[0][0].shape[2]
        rows = parts[0].shape[2]
        sum_shape = (rows, width)
        dims = (((0,), (0,)), ((), ()))
    out_shape = out or jax.ShapeDtypeStruct((chip_experts, *sum_shape), jnp.float32)

    def body(table_ref, *refs):
        part_refs, rest = refs[:n_parts], refs[n_parts:]
        weight_refs, rest = rest[: 2 * n_kinds], rest[2 * n_kinds :]
        extra_refs, out_ref = rest[:-1], rest[-1]
        for e in range(chip_experts):
            side = (e // exp_dev) ^ (0 if ours_first else 1)
            sums = []
            for k in range(n_kinds):
                ref = weight_refs[2 * k + side]
                if into:
                    total = [x[e, k * hid : (k + 1) * hid] for x in extra_refs]
                else:
                    total = [x[e] for x in extra_refs]
                for part_ref, step in zip(part_refs, steps):
                    if into:
                        at = pl.ds(pl.multiple_of(table_ref[step] * width, width), width)
                        pair = (ref[e % exp_dev, :, at], part_ref[e])
                    else:
                        at = pl.ds(pl.multiple_of(table_ref[step] * hid, hid), hid)
                        pair = (part_ref[e], ref[e % exp_dev, at, :])
                    total.append(lax.dot_general(*pair, dims, preferred_element_type=jnp.float32))
                sums.append(sum(total[1:], total[0]))
            if finish is not None:
                finish(out_ref, e, *sums)
            elif into:
                for k, total in enumerate(sums):
                    out_ref[e, k * hid : (k + 1) * hid] = total
            else:
                out_ref[e] = sums[0]

    whole = pl.BlockSpec(memory_space=pltpu.VMEM)
    operands = [*parts, *(w for pair in weights for w in pair), *extra]
    flops = 2 * chip_experts * n_parts * n_kinds * rows * hid * width
    moved = 2 * sum(x.size for x in operands)
    return pl.pallas_call(
        body,
        in_specs=[pl.BlockSpec(memory_space=pltpu.SMEM)] + [whole] * len(operands),
        out_specs=whole,
        out_shape=out_shape,
        compiler_params=pltpu.CompilerParams(vmem_limit_bytes=24 * 2**20),
        cost_estimate=pl.CostEstimate(flops=flops, bytes_accessed=moved, transcendentals=0),
    )(table, *operands)


def gather_sum(own, weights, table, kind, finish, out):
    half = lax.axis_size("dp") // 2
    mine = [own]
    for _ in range(1, half + 1):
        mine.append(onward(mine[-1]))
    other = [swap(own)]
    for _ in range(1, half):
        other.append(onward(other[-1]))
    early = weighted_sum(mine[:half], range(half), weights, table, kind, True)
    aside = weighted_sum(other[1:], range(1, half), weights, table, kind, False)
    back = swap(aside)
    return weighted_sum(mine[half:], [half], weights, table, kind, True, (early, back), finish, out)


def layer(tokens, expert_ids, gate_levels, gate_weight, up_weight, down_weight):
    tok_dev, width = tokens.shape
    picks = expert_ids.shape[1]
    exp_dev = gate_weight.shape[0]
    hid = gate_weight.shape[2]
    n_z = lax.axis_size("z")
    chip_experts = exp_dev * CORES
    experts = chip_experts * n_z
    capacity = min(tok_dev, max(2, 2 * tok_dev * picks // experts))
    core = lax.axis_index("core")
    z = lax.axis_index("z")

    ids_rows = jnp.zeros((2 * picks, width), jnp.bfloat16)
    ids_rows = ids_rows.at[:picks, :tok_dev].set(expert_ids.T.astype(jnp.bfloat16))
    n_dp = lax.axis_size("dp")
    step = jnp.arange(n_dp, dtype=jnp.int32)
    table = (lax.axis_index("dp") + jnp.where(core == 0, -step, step)) % n_dp

    payload = jnp.concatenate([tokens, ids_rows], axis=0)
    payload, table = lax.optimization_barrier((payload, table))
    gathered = lax.all_gather(payload, "z", axis=0)
    all_tokens = gathered[:, :tok_dev]
    all_ids = gathered[:, tok_dev : tok_dev + picks, :tok_dev].astype(jnp.int32)

    local = jnp.arange(chip_experts, dtype=jnp.int32)
    names = z * chip_experts + (local + core * exp_dev) % chip_experts
    member = jnp.any(all_ids[:, None, :, :] == names[None, :, None, None], axis=2)
    spot = jnp.where(member, positions(member), -1)
    chosen = spot[:, :, None, :] == jnp.arange(capacity, dtype=jnp.int32)[None, None, :, None]
    rows = jnp.einsum(
        "sepj,sjd->espd",
        chosen.astype(jnp.bfloat16),
        all_tokens,
        preferred_element_type=jnp.float32,
    ).astype(jnp.bfloat16)
    count = n_z * capacity
    rows = rows.reshape(chip_experts, count, width)

    pairs = []
    for weights in (jnp.swapaxes(gate_weight, 1, 2), jnp.swapaxes(up_weight, 1, 2), down_weight):
        pairs.append((weights, swap(weights)))

    def gated(out_ref, e, gate_sum, up_sum):
        out_ref[e] = (gate_sum / (1.0 + jnp.exp(-gate_sum)) * up_sum).astype(jnp.bfloat16)

    hidden = gather_sum(
        rows,
        pairs[:2],
        table,
        "in",
        gated,
        jax.ShapeDtypeStruct((chip_experts, hid, count), jnp.bfloat16),
    )

    out_features = down_weight.shape[2]

    def returning(out_ref, e, total):
        out_ref[:, e] = total.astype(jnp.bfloat16).reshape(n_z, capacity, out_features)

    result = gather_sum(
        hidden,
        pairs[2:],
        table,
        "out",
        returning,
        jax.ShapeDtypeStruct((n_z, chip_experts, capacity, out_features), jnp.bfloat16),
    )
    returned = lax.all_to_all(result, "z", split_axis=0, concat_axis=0, tiled=True)
    slot_count = experts * capacity
    returned = returned.reshape(slot_count, out_features)

    own_ids = expert_ids.T
    every = jnp.arange(experts, dtype=jnp.int32)
    in_chip = every % chip_experts
    names = every - in_chip + (in_chip + core * exp_dev) % chip_experts
    named = own_ids[None, :, :] == names[:, None, None]
    own_spot = positions(jnp.any(named, axis=1))
    shares = gate_levels.astype(jnp.float32) / 256.0
    factor = jnp.sum(jnp.where(named, shares.T[None, :, :], 0.0), axis=1)
    weighting = jnp.where(
        own_spot[:, None, :] == jnp.arange(capacity, dtype=jnp.int32)[None, :, None],
        factor[:, None, :],
        0.0,
    ).astype(jnp.bfloat16)
    weighting = weighting.reshape(slot_count, tok_dev)
    combined = jnp.einsum("sj,sd->jd", weighting, returned, preferred_element_type=jnp.float32)
    return combined.astype(jnp.bfloat16)


def solution(mesh):
    groups, expert, dp = (mesh.shape[name] for name in ("groups", "expert", "dp"))
    split = Mesh(
        mesh.devices.reshape(groups, expert // CORES, CORES, dp), ("groups", "z", "core", "dp")
    )
    rows, held = ("groups", "z", "core"), ("z", "core")
    in_specs = (
        P(rows, "dp"),
        P(rows, None),
        P(rows, None),
        P(held, None, "dp"),
        P(held, None, "dp"),
        P(held, None, "dp"),
    )
    return jax.shard_map(
        layer, mesh=split, in_specs=in_specs, out_specs=P(rows, "dp"), check_vma=False
    )
```

```python
import jax
import jax.numpy as jnp
from jax import lax
from jax.experimental import pallas as pl
from jax.experimental.pallas import tpu as pltpu
from jax.sharding import Mesh, PartitionSpec as P


CORES = 2


def swap(block):
    return lax.ppermute(block, "core", [(0, 1), (1, 0)])


def onward(block):
    count = lax.axis_size("dp")
    up = [(i, (i + 1) % count) for i in range(count)]
    down = [(count + i, count + (i - 1) % count) for i in range(count)]
    return lax.ppermute(block, ("core", "dp"), up + down)


def positions(member):
    count = member.shape[-1]
    row = lax.broadcasted_iota(jnp.int32, (count, count), 0)
    col = lax.broadcasted_iota(jnp.int32, (count, count), 1)
    before = (row < col).astype(jnp.bfloat16)
    return jnp.einsum(
        "...i,ij->...j", member.astype(jnp.bfloat16), before, preferred_element_type=jnp.float32
    ).astype(jnp.int32)


def chosen_rows(gathered, first, turn, tok_dev, picks, chip_experts, capacity):
    sources, _, width = gathered.shape
    slots = chip_experts * capacity

    def body(table_ref, gathered_ref, out_ref):
        row = lax.broadcasted_iota(jnp.int32, (tok_dev, tok_dev), 0)
        col = lax.broadcasted_iota(jnp.int32, (tok_dev, tok_dev), 1)
        before = (row < col).astype(jnp.bfloat16)
        lines = []
        for s in range(sources):
            ids = gathered_ref[s, tok_dev : tok_dev + picks, :tok_dev].astype(jnp.float32)
            for e in range(chip_experts):
                name = table_ref[0] + lax.rem(table_ref[1] + e, chip_experts)
                same = jnp.where(ids == name.astype(jnp.float32), 1.0, 0.0)
                lines.append(jnp.max(same, axis=0, keepdims=True))
        member = jnp.concatenate(lines, axis=0)
        spot = lax.dot_general(
            member.astype(jnp.bfloat16),
            before,
            (((1,), (0,)), ((), ())),
            preferred_element_type=jnp.float32,
        )
        spot = jnp.where(member > 0.5, spot, -1.0)
        slot = lax.broadcasted_iota(jnp.int32, (capacity, tok_dev), 0).astype(jnp.float32)
        for s in range(sources):
            picked = [
                jnp.where(spot[at : at + 1] == slot, 1.0, 0.0)
                for at in range(s * chip_experts, (s + 1) * chip_experts)
            ]
            found = lax.dot_general(
                jnp.concatenate(picked, axis=0).astype(jnp.bfloat16),
                gathered_ref[s, :tok_dev],
                (((1,), (0,)), ((), ())),
                preferred_element_type=jnp.float32,
            ).astype(jnp.bfloat16)
            for e in range(chip_experts):
                out_ref[e, s * capacity : (s + 1) * capacity] = found[
                    e * capacity : (e + 1) * capacity
                ]

    table = jnp.stack([first, turn]).astype(jnp.int32)
    return pl.pallas_call(
        body,
        in_specs=[pl.BlockSpec(memory_space=pltpu.SMEM), pl.BlockSpec(memory_space=pltpu.VMEM)],
        out_specs=pl.BlockSpec(memory_space=pltpu.VMEM),
        out_shape=jax.ShapeDtypeStruct((chip_experts, sources * capacity, width), jnp.bfloat16),
        compiler_params=pltpu.CompilerParams(vmem_limit_bytes=16 * 2**20),
        cost_estimate=pl.CostEstimate(
            flops=2 * sources * slots * tok_dev * width,
            bytes_accessed=2 * gathered.size,
            transcendentals=0,
        ),
    )(table, gathered)


def weighted_sum(parts, steps, weights, table, kind, ours_first, extra=(), finish=None, out=None):
    chip_experts = parts[0].shape[0]
    exp_dev = weights[0][0].shape[0]
    n_parts, n_kinds = len(parts), len(weights)
    into = kind == "in"
    if into:
        hid, width = weights[0][0].shape[1], parts[0].shape[2]
        rows = parts[0].shape[1]
        sum_shape = (n_kinds * hid, rows)
        dims = (((1,), (1,)), ((), ()))
    else:
        hid, width = parts[0].shape[1], weights[0][0].shape[2]
        rows = parts[0].shape[2]
        sum_shape = (rows, width)
        dims = (((0,), (0,)), ((), ()))
    out_shape = out or jax.ShapeDtypeStruct((chip_experts, *sum_shape), jnp.float32)

    def body(table_ref, *refs):
        part_refs, rest = refs[:n_parts], refs[n_parts:]
        weight_refs, rest = rest[: 2 * n_kinds], rest[2 * n_kinds :]
        extra_refs, out_ref = rest[:-1], rest[-1]
        for e in range(chip_experts):
            side = (e // exp_dev) ^ (0 if ours_first else 1)
            sums = []
            for k in range(n_kinds):
                ref = weight_refs[2 * k + side]
                if into:
                    total = [x[e, k * hid : (k + 1) * hid] for x in extra_refs]
                else:
                    total = [x[e] for x in extra_refs]
                for part_ref, step in zip(part_refs, steps):
                    if into:
                        at = pl.ds(pl.multiple_of(table_ref[step] * width, width), width)
                        pair = (ref[e % exp_dev, :, at], part_ref[e])
                    else:
                        at = pl.ds(pl.multiple_of(table_ref[step] * hid, hid), hid)
                        pair = (part_ref[e], ref[e % exp_dev, at, :])
                    total.append(lax.dot_general(*pair, dims, preferred_element_type=jnp.float32))
                sums.append(sum(total[1:], total[0]))
            if finish is not None:
                finish(out_ref, e, *sums)
            elif into:
                for k, total in enumerate(sums):
                    out_ref[e, k * hid : (k + 1) * hid] = total
            else:
                out_ref[e] = sums[0]

    whole = pl.BlockSpec(memory_space=pltpu.VMEM)
    operands = [*parts, *(w for pair in weights for w in pair), *extra]
    flops = 2 * chip_experts * n_parts * n_kinds * rows * hid * width
    moved = 2 * sum(x.size for x in operands)
    return pl.pallas_call(
        body,
        in_specs=[pl.BlockSpec(memory_space=pltpu.SMEM)] + [whole] * len(operands),
        out_specs=whole,
        out_shape=out_shape,
        compiler_params=pltpu.CompilerParams(vmem_limit_bytes=24 * 2**20),
        cost_estimate=pl.CostEstimate(flops=flops, bytes_accessed=moved, transcendentals=0),
    )(table, *operands)


def gather_sum(own, weights, table, kind, finish, out):
    half = lax.axis_size("dp") // 2
    mine = [own]
    for _ in range(1, half + 1):
        mine.append(onward(mine[-1]))
    other = [swap(own)]
    for _ in range(1, half):
        other.append(onward(other[-1]))
    early = weighted_sum(mine[:half], range(half), weights, table, kind, True)
    aside = weighted_sum(other[1:], range(1, half), weights, table, kind, False)
    back = swap(aside)
    return weighted_sum(mine[half:], [half], weights, table, kind, True, (early, back), finish, out)


def layer(tokens, expert_ids, gate_levels, gate_weight, up_weight, down_weight):
    tok_dev, width = tokens.shape
    picks = expert_ids.shape[1]
    exp_dev = gate_weight.shape[0]
    hid = gate_weight.shape[2]
    n_z = lax.axis_size("z")
    chip_experts = exp_dev * CORES
    experts = chip_experts * n_z
    capacity = min(tok_dev, max(2, 2 * tok_dev * picks // experts))
    core = lax.axis_index("core")
    z = lax.axis_index("z")

    ids_rows = jnp.zeros((2 * picks, width), jnp.bfloat16)
    ids_rows = ids_rows.at[:picks, :tok_dev].set(expert_ids.T.astype(jnp.bfloat16))
    n_dp = lax.axis_size("dp")
    step = jnp.arange(n_dp, dtype=jnp.int32)
    table = (lax.axis_index("dp") + jnp.where(core == 0, -step, step)) % n_dp

    payload = jnp.concatenate([tokens, ids_rows], axis=0)
    payload, table = lax.optimization_barrier((payload, table))
    gathered = lax.all_gather(payload, "z", axis=0)
    count = n_z * capacity
    rows = chosen_rows(gathered, z * chip_experts, core * exp_dev, tok_dev, picks, chip_experts, capacity)

    pairs = []
    for weights in (jnp.swapaxes(gate_weight, 1, 2), jnp.swapaxes(up_weight, 1, 2), down_weight):
        pairs.append((weights, swap(weights)))

    def gated(out_ref, e, gate_sum, up_sum):
        out_ref[e] = (gate_sum / (1.0 + jnp.exp(-gate_sum)) * up_sum).astype(jnp.bfloat16)

    hidden = gather_sum(
        rows,
        pairs[:2],
        table,
        "in",
        gated,
        jax.ShapeDtypeStruct((chip_experts, hid, count), jnp.bfloat16),
    )

    out_features = down_weight.shape[2]

    def returning(out_ref, e, total):
        out_ref[:, e] = total.astype(jnp.bfloat16).reshape(n_z, capacity, out_features)

    result = gather_sum(
        hidden,
        pairs[2:],
        table,
        "out",
        returning,
        jax.ShapeDtypeStruct((n_z, chip_experts, capacity, out_features), jnp.bfloat16),
    )
    returned = lax.all_to_all(result, "z", split_axis=0, concat_axis=0, tiled=True)
    slot_count = experts * capacity
    returned = returned.reshape(slot_count, out_features)

    own_ids = expert_ids.T
    every = jnp.arange(experts, dtype=jnp.int32)
    in_chip = every % chip_experts
    names = every - in_chip + (in_chip + core * exp_dev) % chip_experts
    named = own_ids[None, :, :] == names[:, None, None]
    own_spot = positions(jnp.any(named, axis=1))
    shares = gate_levels.astype(jnp.float32) / 256.0
    factor = jnp.sum(jnp.where(named, shares.T[None, :, :], 0.0), axis=1)
    weighting = jnp.where(
        own_spot[:, None, :] == jnp.arange(capacity, dtype=jnp.int32)[None, :, None],
        factor[:, None, :],
        0.0,
    ).astype(jnp.bfloat16)
    weighting = weighting.reshape(slot_count, tok_dev)
    combined = jnp.einsum("sj,sd->jd", weighting, returned, preferred_element_type=jnp.float32)
    return combined.astype(jnp.bfloat16)


def solution(mesh):
    groups, expert, dp = (mesh.shape[name] for name in ("groups", "expert", "dp"))
    split = Mesh(
        mesh.devices.reshape(groups, expert // CORES, CORES, dp), ("groups", "z", "core", "dp")
    )
    rows, held = ("groups", "z", "core"), ("z", "core")
    in_specs = (
        P(rows, "dp"),
        P(rows, None),
        P(rows, None),
        P(held, None, "dp"),
        P(held, None, "dp"),
        P(held, None, "dp"),
    )
    return jax.shard_map(
        layer, mesh=split, in_specs=in_specs, out_specs=P(rows, "dp"), check_vma=False
    )
```

```python
import jax
import jax.numpy as jnp
from jax import lax
from jax.experimental import pallas as pl
from jax.experimental.pallas import tpu as pltpu
from jax.sharding import Mesh, PartitionSpec as P


CORES = 2


def swap(block):
    return lax.ppermute(block, "core", [(0, 1), (1, 0)])


def shift(block, step):
    count = lax.axis_size("dp")
    return lax.ppermute(block, "dp", [(i, (i + step) % count) for i in range(count)])


def onward(block):
    count = lax.axis_size("dp")
    up = [(i, (i + 1) % count) for i in range(count)]
    down = [(count + i, count + (i - 1) % count) for i in range(count)]
    return lax.ppermute(block, ("core", "dp"), up + down)


def positions(member):
    count = member.shape[-1]
    row = lax.broadcasted_iota(jnp.int32, (count, count), 0)
    col = lax.broadcasted_iota(jnp.int32, (count, count), 1)
    before = (row < col).astype(jnp.bfloat16)
    return jnp.einsum(
        "...i,ij->...j", member.astype(jnp.bfloat16), before, preferred_element_type=jnp.float32
    ).astype(jnp.int32)


def with_ids(tokens, ids):
    tok_dev, width = tokens.shape
    picks = ids.shape[0]

    def body(tokens_ref, ids_ref, out_ref):
        out_ref[:tok_dev] = tokens_ref[...]
        found = ids_ref[...].astype(jnp.float32)
        tall = jnp.concatenate([found, jnp.zeros((picks, tok_dev), jnp.float32)], axis=0)
        wide = jnp.concatenate([tall, jnp.zeros((2 * picks, width - tok_dev), jnp.float32)], axis=1)
        out_ref[tok_dev:] = wide.astype(jnp.bfloat16)

    return pl.pallas_call(
        body,
        out_shape=jax.ShapeDtypeStruct((tok_dev + 2 * picks, width), jnp.bfloat16),
        compiler_params=pltpu.CompilerParams(vmem_limit_bytes=4 * 2**20),
        cost_estimate=pl.CostEstimate(flops=2 * tokens.size, bytes_accessed=4 * tokens.size, transcendentals=0),
    )(tokens, ids)


def chosen_rows(gathered, table, tok_dev, picks, chip_experts, capacity):
    sources, _, width = gathered.shape
    slots = chip_experts * capacity
    end = table.shape[0]

    def body(table_ref, gathered_ref, out_ref):
        row = lax.broadcasted_iota(jnp.int32, (tok_dev, tok_dev), 0)
        col = lax.broadcasted_iota(jnp.int32, (tok_dev, tok_dev), 1)
        before = (row < col).astype(jnp.bfloat16)
        lines = []
        for s in range(sources):
            ids = gathered_ref[s, tok_dev : tok_dev + picks, :tok_dev].astype(jnp.float32)
            for e in range(chip_experts):
                name = table_ref[end - 2] + lax.rem(table_ref[end - 1] + e, chip_experts)
                same = jnp.where(ids == name.astype(jnp.float32), 1.0, 0.0)
                lines.append(jnp.max(same, axis=0, keepdims=True))
        member = jnp.concatenate(lines, axis=0)
        spot = lax.dot_general(
            member.astype(jnp.bfloat16),
            before,
            (((1,), (0,)), ((), ())),
            preferred_element_type=jnp.float32,
        )
        spot = jnp.where(member > 0.5, spot, -1.0)
        slot = lax.broadcasted_iota(jnp.int32, (capacity, tok_dev), 0).astype(jnp.float32)
        for s in range(sources):
            picked = [
                jnp.where(spot[at : at + 1] == slot, 1.0, 0.0)
                for at in range(s * chip_experts, (s + 1) * chip_experts)
            ]
            found = lax.dot_general(
                jnp.concatenate(picked, axis=0).astype(jnp.bfloat16),
                gathered_ref[s, :tok_dev],
                (((1,), (0,)), ((), ())),
                preferred_element_type=jnp.float32,
            ).astype(jnp.bfloat16)
            for e in range(chip_experts):
                out_ref[e, s * capacity : (s + 1) * capacity] = found[
                    e * capacity : (e + 1) * capacity
                ]

    return pl.pallas_call(
        body,
        in_specs=[pl.BlockSpec(memory_space=pltpu.SMEM), pl.BlockSpec(memory_space=pltpu.VMEM)],
        out_specs=pl.BlockSpec(memory_space=pltpu.VMEM),
        out_shape=jax.ShapeDtypeStruct((chip_experts, sources * capacity, width), jnp.bfloat16),
        compiler_params=pltpu.CompilerParams(vmem_limit_bytes=16 * 2**20),
        cost_estimate=pl.CostEstimate(
            flops=2 * sources * slots * tok_dev * width,
            bytes_accessed=2 * gathered.size,
            transcendentals=0,
        ),
    )(table, gathered)


def weighted_sum(parts, steps, weights, table, kind, order, extra=(), finish=None, out=None):
    exp_dev = weights[0][0].shape[0]
    chip_experts = exp_dev * CORES
    n_kinds = len(weights)
    into = kind == "in"
    groups, place, flat = [], [], []
    for part in parts:
        blocks = part if isinstance(part, tuple) else (part,)
        holder, first = [], 0
        for block in blocks:
            holder += [len(flat)] * block.shape[0]
            place.append({first + n: n for n in range(block.shape[0])})
            flat.append(block)
            first += block.shape[0]
        groups.append(holder)
    parts, n_parts = flat, len(flat)
    if into:
        hid, width = weights[0][0].shape[1], parts[0].shape[2]
        rows = parts[0].shape[1]
        sum_shape = (n_kinds * hid, rows)
        dims = (((1,), (1,)), ((), ()))
    else:
        hid, width = parts[0].shape[1], weights[0][0].shape[2]
        rows = parts[0].shape[2]
        sum_shape = (rows, width)
        dims = (((0,), (0,)), ((), ()))
    out_shape = out or jax.ShapeDtypeStruct((chip_experts, *sum_shape), jnp.float32)

    def body(table_ref, *refs):
        part_refs, rest = refs[:n_parts], refs[n_parts:]
        weight_refs, rest = rest[: 2 * n_kinds], rest[2 * n_kinds :]
        extra_refs, out_ref = rest[:-1], rest[-1]
        for e in range(chip_experts):
            side = order[e // exp_dev]
            sums = []
            for k in range(n_kinds):
                ref = weight_refs[2 * k + side]
                spot = (slice(k * hid, (k + 1) * hid),) if into else ()
                total = [x[(e, *spot)].astype(jnp.float32) for x in extra_refs]
                for part_refs_of, step in zip(groups, steps):
                    part = part_refs[part_refs_of[e]][place[part_refs_of[e]][e]]
                    if into:
                        at = pl.ds(pl.multiple_of(table_ref[step] * width, width), width)
                        pair = (ref[e % exp_dev, :, at], part)
                    else:
                        at = pl.ds(pl.multiple_of(table_ref[step] * hid, hid), hid)
                        pair = (part, ref[e % exp_dev, at, :])
                    total.append(lax.dot_general(*pair, dims, preferred_element_type=jnp.float32))
                sums.append(sum(total[1:], total[0]))
            if finish is not None:
                finish(out_ref, e, *sums)
            elif into:
                for k, total in enumerate(sums):
                    out_ref[e, k * hid : (k + 1) * hid] = total.astype(out_ref.dtype)
            else:
                out_ref[e] = sums[0].astype(out_ref.dtype)

    whole = pl.BlockSpec(memory_space=pltpu.VMEM)
    operands = [*parts, *(w for pair in weights for w in pair), *extra]
    flops = 2 * chip_experts * n_parts * n_kinds * rows * hid * width
    moved = 2 * sum(x.size for x in operands)
    return pl.pallas_call(
        body,
        in_specs=[pl.BlockSpec(memory_space=pltpu.SMEM)] + [whole] * len(operands),
        out_specs=whole,
        out_shape=out_shape,
        compiler_params=pltpu.CompilerParams(vmem_limit_bytes=24 * 2**20),
        cost_estimate=pl.CostEstimate(flops=flops, bytes_accessed=moved, transcendentals=0),
    )(table, *operands)


def tokens_sum(own, weights, owners, finish, out):
    half = lax.axis_size("dp") // 2
    mine = [own]
    for _ in range(1, half + 1):
        mine.append(onward(mine[-1]))
    other = [swap(own)]
    for _ in range(1, half):
        other.append(onward(other[-1]))
    early = weighted_sum(mine[: half - 1], range(half - 1), weights, owners, "in", (0, 1))
    ahead = weighted_sum(
        other[1 : half - 1], range(1, half - 1), weights, owners, "in", (1, 0)
    )
    sums = jax.ShapeDtypeStruct(ahead.shape, jnp.bfloat16)
    aside = weighted_sum(
        other[half - 1 :], [half - 1], weights, owners, "in", (1, 0), (ahead,), None, sums
    )
    back = swap(aside)
    return weighted_sum(
        mine[half - 1 :],
        [half - 1, half],
        weights,
        owners,
        "in",
        (0, 1),
        (early, back),
        finish,
        out,
    )


def hidden_sum(own, weights, owners, finish, out):
    count = lax.axis_size("dp")
    half = count // 2
    up, down = [own], [own]
    for _ in range(1, half):
        up.append(shift(up[-1], 1))
        down.append(shift(down[-1], -1))
    middle = own.shape[0] // 2
    last_up = shift(up[-1][:middle], 1)
    last_down = shift(down[-1][middle:], -1)
    steps = [*range(count, count + half), *(2 * count - step for step in range(1, half))]
    early = weighted_sum([*up, *down[1:]], steps, weights, owners, "out", (0, 1))
    return weighted_sum(
        [(last_up, last_down)], [count + half], weights, owners, "out", (0, 1), (early,), finish, out
    )


def layer(tokens, expert_ids, gate_levels, gate_weight, up_weight, down_weight):
    tok_dev, _ = tokens.shape
    picks = expert_ids.shape[1]
    exp_dev = gate_weight.shape[0]
    hid = gate_weight.shape[2]
    n_z = lax.axis_size("z")
    chip_experts = exp_dev * CORES
    experts = chip_experts * n_z
    capacity = min(tok_dev, max(2, 2 * tok_dev * picks // experts))
    core = lax.axis_index("core")
    z = lax.axis_index("z")

    n_dp = lax.axis_size("dp")
    at = jnp.arange(2 * n_dp + 2, dtype=jnp.int32)
    me = lax.axis_index("dp")
    turn = jnp.where((core == 1) & (at < n_dp), 1, -1)
    table = (me + turn * (at % n_dp)) % n_dp
    table = jnp.where(at == 2 * n_dp, z * chip_experts, table)
    table = jnp.where(at == 2 * n_dp + 1, core * exp_dev, table)

    payload = with_ids(tokens, expert_ids.T)
    payload, table = lax.optimization_barrier((payload, table))
    gathered = lax.all_gather(payload, "z", axis=0)
    count = n_z * capacity
    rows = chosen_rows(gathered, table, tok_dev, picks, chip_experts, capacity)

    pairs = []
    for weights in (jnp.swapaxes(gate_weight, 1, 2), jnp.swapaxes(up_weight, 1, 2), down_weight):
        pairs.append((weights, swap(weights)))

    def gated(out_ref, e, gate_sum, up_sum):
        out_ref[e] = (gate_sum / (1.0 + jnp.exp(-gate_sum)) * up_sum).astype(jnp.bfloat16)

    hidden = tokens_sum(
        rows,
        pairs[:2],
        table,
        gated,
        jax.ShapeDtypeStruct((chip_experts, hid, count), jnp.bfloat16),
    )

    out_features = down_weight.shape[2]

    def returning(out_ref, e, total):
        out_ref[:, e] = total.astype(jnp.bfloat16).reshape(n_z, capacity, out_features)

    result = hidden_sum(
        hidden,
        pairs[2:],
        table,
        returning,
        jax.ShapeDtypeStruct((n_z, chip_experts, capacity, out_features), jnp.bfloat16),
    )
    returned = lax.all_to_all(result, "z", split_axis=0, concat_axis=0, tiled=True)
    slot_count = experts * capacity
    returned = returned.reshape(slot_count, out_features)

    own_ids = expert_ids.T
    every = jnp.arange(experts, dtype=jnp.int32)
    in_chip = every % chip_experts
    names = every - in_chip + (in_chip + core * exp_dev) % chip_experts
    named = own_ids[None, :, :] == names[:, None, None]
    own_spot = positions(jnp.any(named, axis=1))
    shares = gate_levels.astype(jnp.float32) / 256.0
    factor = jnp.sum(jnp.where(named, shares.T[None, :, :], 0.0), axis=1)
    weighting = jnp.where(
        own_spot[:, None, :] == jnp.arange(capacity, dtype=jnp.int32)[None, :, None],
        factor[:, None, :],
        0.0,
    ).astype(jnp.bfloat16)
    weighting = weighting.reshape(slot_count, tok_dev)
    combined = jnp.einsum("sj,sd->jd", weighting, returned, preferred_element_type=jnp.float32)
    return combined.astype(jnp.bfloat16)


def solution(mesh):
    groups, expert, dp = (mesh.shape[name] for name in ("groups", "expert", "dp"))
    split = Mesh(
        mesh.devices.reshape(groups, expert // CORES, CORES, dp), ("groups", "z", "core", "dp")
    )
    rows, held = ("groups", "z", "core"), ("z", "core")
    in_specs = (
        P(rows, "dp"),
        P(rows, None),
        P(rows, None),
        P(held, None, "dp"),
        P(held, None, "dp"),
        P(held, None, "dp"),
    )
    return jax.shard_map(
        layer, mesh=split, in_specs=in_specs, out_specs=P(rows, "dp"), check_vma=False
    )
```

```python
import jax
import jax.numpy as jnp
from jax import lax
from jax.experimental import pallas as pl
from jax.experimental.pallas import tpu as pltpu
from jax.sharding import Mesh, PartitionSpec as P


CORES = 2


def swap(block):
    return lax.ppermute(block, "core", [(0, 1), (1, 0)])


def onward(block):
    count = lax.axis_size("dp")
    up = [(i, (i + 1) % count) for i in range(count)]
    down = [(count + i, count + (i - 1) % count) for i in range(count)]
    return lax.ppermute(block, ("core", "dp"), up + down)


def positions(member):
    count = member.shape[-1]
    row = lax.broadcasted_iota(jnp.int32, (count, count), 0)
    col = lax.broadcasted_iota(jnp.int32, (count, count), 1)
    before = (row < col).astype(jnp.bfloat16)
    return jnp.einsum(
        "...i,ij->...j", member.astype(jnp.bfloat16), before, preferred_element_type=jnp.float32
    ).astype(jnp.int32)


def with_ids(tokens, ids):
    tok_dev, width = tokens.shape
    picks = ids.shape[0]

    def body(tokens_ref, ids_ref, out_ref):
        out_ref[:tok_dev] = tokens_ref[...]
        found = ids_ref[...].astype(jnp.float32)
        tall = jnp.concatenate([found, jnp.zeros((picks, tok_dev), jnp.float32)], axis=0)
        wide = jnp.concatenate([tall, jnp.zeros((2 * picks, width - tok_dev), jnp.float32)], axis=1)
        out_ref[tok_dev:] = wide.astype(jnp.bfloat16)

    return pl.pallas_call(
        body,
        out_shape=jax.ShapeDtypeStruct((tok_dev + 2 * picks, width), jnp.bfloat16),
        compiler_params=pltpu.CompilerParams(vmem_limit_bytes=4 * 2**20),
        cost_estimate=pl.CostEstimate(flops=2 * tokens.size, bytes_accessed=4 * tokens.size, transcendentals=0),
    )(tokens, ids)


def chosen_rows(gathered, table, tok_dev, picks, chip_experts, capacity):
    sources, _, width = gathered.shape
    slots = chip_experts * capacity
    end = table.shape[0]

    def body(table_ref, gathered_ref, out_ref):
        row = lax.broadcasted_iota(jnp.int32, (tok_dev, tok_dev), 0)
        col = lax.broadcasted_iota(jnp.int32, (tok_dev, tok_dev), 1)
        before = (row < col).astype(jnp.bfloat16)
        lines = []
        for s in range(sources):
            ids = gathered_ref[s, tok_dev : tok_dev + picks, :tok_dev].astype(jnp.float32)
            for e in range(chip_experts):
                name = table_ref[end - 2] + lax.rem(table_ref[end - 1] + e, chip_experts)
                same = jnp.where(ids == name.astype(jnp.float32), 1.0, 0.0)
                lines.append(jnp.max(same, axis=0, keepdims=True))
        member = jnp.concatenate(lines, axis=0)
        spot = lax.dot_general(
            member.astype(jnp.bfloat16),
            before,
            (((1,), (0,)), ((), ())),
            preferred_element_type=jnp.float32,
        )
        spot = jnp.where(member > 0.5, spot, -1.0)
        slot = lax.broadcasted_iota(jnp.int32, (capacity, tok_dev), 0).astype(jnp.float32)
        for s in range(sources):
            picked = [
                jnp.where(spot[at : at + 1] == slot, 1.0, 0.0)
                for at in range(s * chip_experts, (s + 1) * chip_experts)
            ]
            found = lax.dot_general(
                jnp.concatenate(picked, axis=0).astype(jnp.bfloat16),
                gathered_ref[s, :tok_dev],
                (((1,), (0,)), ((), ())),
                preferred_element_type=jnp.float32,
            ).astype(jnp.bfloat16)
            for e in range(chip_experts):
                out_ref[e, s * capacity : (s + 1) * capacity] = found[
                    e * capacity : (e + 1) * capacity
                ]

    return pl.pallas_call(
        body,
        in_specs=[pl.BlockSpec(memory_space=pltpu.SMEM), pl.BlockSpec(memory_space=pltpu.VMEM)],
        out_specs=pl.BlockSpec(memory_space=pltpu.VMEM),
        out_shape=jax.ShapeDtypeStruct((chip_experts, sources * capacity, width), jnp.bfloat16),
        compiler_params=pltpu.CompilerParams(vmem_limit_bytes=16 * 2**20),
        cost_estimate=pl.CostEstimate(
            flops=2 * sources * slots * tok_dev * width,
            bytes_accessed=2 * gathered.size,
            transcendentals=0,
        ),
    )(table, gathered)


def weighted_sum(parts, steps, weights, table, kind, order, extra=(), finish=None, out=None):
    exp_dev = weights[0][0].shape[0]
    chip_experts = exp_dev * CORES
    n_kinds = len(weights)
    into = kind == "in"
    n_parts = len(parts)
    if into:
        hid, width = weights[0][0].shape[1], parts[0].shape[2]
        rows = parts[0].shape[1]
        sum_shape = (n_kinds * hid, rows)
        dims = (((1,), (1,)), ((), ()))
    else:
        hid, width = parts[0].shape[1], weights[0][0].shape[2]
        rows = parts[0].shape[2]
        sum_shape = (rows, width)
        dims = (((0,), (0,)), ((), ()))
    out_shape = out or jax.ShapeDtypeStruct((chip_experts, *sum_shape), jnp.float32)

    def body(table_ref, *refs):
        part_refs, rest = refs[:n_parts], refs[n_parts:]
        weight_refs, rest = rest[: 2 * n_kinds], rest[2 * n_kinds :]
        extra_refs, out_ref = rest[:-1], rest[-1]
        for e in range(chip_experts):
            side = order[e // exp_dev]
            sums = []
            for k in range(n_kinds):
                ref = weight_refs[2 * k + side]
                spot = (slice(k * hid, (k + 1) * hid),) if into else ()
                total = [x[(e, *spot)].astype(jnp.float32) for x in extra_refs]
                for part_ref, step in zip(part_refs, steps):
                    part = part_ref[e]
                    if into:
                        at = pl.ds(pl.multiple_of(table_ref[step] * width, width), width)
                        pair = (ref[e % exp_dev, :, at], part)
                    else:
                        at = pl.ds(pl.multiple_of(table_ref[step] * hid, hid), hid)
                        pair = (part, ref[e % exp_dev, at, :])
                    total.append(lax.dot_general(*pair, dims, preferred_element_type=jnp.float32))
                sums.append(sum(total[1:], total[0]))
            if finish is not None:
                finish(out_ref, e, *sums)
            elif into:
                for k, total in enumerate(sums):
                    out_ref[e, k * hid : (k + 1) * hid] = total.astype(out_ref.dtype)
            else:
                out_ref[e] = sums[0].astype(out_ref.dtype)

    whole = pl.BlockSpec(memory_space=pltpu.VMEM)
    operands = [*parts, *(w for pair in weights for w in pair), *extra]
    flops = 2 * chip_experts * n_parts * n_kinds * rows * hid * width
    moved = 2 * sum(x.size for x in operands)
    return pl.pallas_call(
        body,
        in_specs=[pl.BlockSpec(memory_space=pltpu.SMEM)] + [whole] * len(operands),
        out_specs=whole,
        out_shape=out_shape,
        compiler_params=pltpu.CompilerParams(vmem_limit_bytes=24 * 2**20),
        cost_estimate=pl.CostEstimate(flops=flops, bytes_accessed=moved, transcendentals=0),
    )(table, *operands)


def gather_sum(own, weights, owners, kind, finish, out):
    half = lax.axis_size("dp") // 2
    summed = lambda parts, steps, order, *rest: weighted_sum(
        parts, steps, weights, owners, kind, order, *rest
    )
    mine = [own]
    for _ in range(1, half + 1):
        mine.append(onward(mine[-1]))
    other = [swap(own)]
    for _ in range(1, half):
        other.append(onward(other[-1]))
    early = summed(mine[: half - 1], range(half - 1), (0, 1))
    ahead = summed(other[1 : half - 1], range(1, half - 1), (1, 0))
    aside = summed(other[half - 1 :], [half - 1], (1, 0), (ahead,))
    back = swap(aside)
    return summed(mine[half - 1 :], [half - 1, half], (0, 1), (early, back), finish, out)


def layer(tokens, expert_ids, gate_levels, gate_weight, up_weight, down_weight):
    tok_dev, _ = tokens.shape
    picks = expert_ids.shape[1]
    exp_dev = gate_weight.shape[0]
    hid = gate_weight.shape[2]
    n_z = lax.axis_size("z")
    chip_experts = exp_dev * CORES
    experts = chip_experts * n_z
    capacity = min(tok_dev, max(2, 2 * tok_dev * picks // experts))
    core = lax.axis_index("core")
    z = lax.axis_index("z")

    n_dp = lax.axis_size("dp")
    at = jnp.arange(n_dp + 2, dtype=jnp.int32)
    table = (lax.axis_index("dp") + jnp.where(core == 1, at, -at)) % n_dp
    table = jnp.where(at == n_dp, z * chip_experts, table)
    table = jnp.where(at == n_dp + 1, core * exp_dev, table)

    payload = with_ids(tokens, expert_ids.T)
    payload, table = lax.optimization_barrier((payload, table))
    gathered = lax.all_gather(payload, "z", axis=0)
    count = n_z * capacity
    rows = chosen_rows(gathered, table, tok_dev, picks, chip_experts, capacity)

    pairs = []
    for weights in (jnp.swapaxes(gate_weight, 1, 2), jnp.swapaxes(up_weight, 1, 2), down_weight):
        pairs.append((weights, swap(weights)))

    def gated(out_ref, e, gate_sum, up_sum):
        out_ref[e] = (gate_sum / (1.0 + jnp.exp(-gate_sum)) * up_sum).astype(jnp.bfloat16)

    hidden = gather_sum(
        rows,
        pairs[:2],
        table,
        "in",
        gated,
        jax.ShapeDtypeStruct((chip_experts, hid, count), jnp.bfloat16),
    )

    out_features = down_weight.shape[2]

    def returning(out_ref, e, total):
        out_ref[:, e] = total.astype(jnp.bfloat16).reshape(n_z, capacity, out_features)

    result = gather_sum(
        hidden,
        pairs[2:],
        table,
        "out",
        returning,
        jax.ShapeDtypeStruct((n_z, chip_experts, capacity, out_features), jnp.bfloat16),
    )
    returned = lax.all_to_all(result, "z", split_axis=0, concat_axis=0, tiled=True)
    slot_count = experts * capacity
    returned = returned.reshape(slot_count, out_features)

    own_ids = expert_ids.T
    every = jnp.arange(experts, dtype=jnp.int32)
    in_chip = every % chip_experts
    names = every - in_chip + (in_chip + core * exp_dev) % chip_experts
    named = own_ids[None, :, :] == names[:, None, None]
    own_spot = positions(jnp.any(named, axis=1))
    shares = gate_levels.astype(jnp.float32) / 256.0
    factor = jnp.sum(jnp.where(named, shares.T[None, :, :], 0.0), axis=1)
    weighting = jnp.where(
        own_spot[:, None, :] == jnp.arange(capacity, dtype=jnp.int32)[None, :, None],
        factor[:, None, :],
        0.0,
    ).astype(jnp.bfloat16)
    weighting = weighting.reshape(slot_count, tok_dev)
    combined = jnp.einsum("sj,sd->jd", weighting, returned, preferred_element_type=jnp.float32)
    return combined.astype(jnp.bfloat16)


def solution(mesh):
    groups, expert, dp = (mesh.shape[name] for name in ("groups", "expert", "dp"))
    split = Mesh(
        mesh.devices.reshape(groups, expert // CORES, CORES, dp), ("groups", "z", "core", "dp")
    )
    rows, held = ("groups", "z", "core"), ("z", "core")
    in_specs = (
        P(rows, "dp"),
        P(rows, None),
        P(rows, None),
        P(held, None, "dp"),
        P(held, None, "dp"),
        P(held, None, "dp"),
    )
    return jax.shard_map(
        layer, mesh=split, in_specs=in_specs, out_specs=P(rows, "dp"), check_vma=False
    )
```

```python
import jax
import jax.numpy as jnp
from jax import lax
from jax.experimental import pallas as pl
from jax.experimental.pallas import tpu as pltpu
from jax.sharding import Mesh, PartitionSpec as P


CORES = 2


def swap(block):
    return lax.ppermute(block, "core", [(0, 1), (1, 0)])


def onward(block):
    count = lax.axis_size("dp")
    up = [(i, (i + 1) % count) for i in range(count)]
    down = [(count + i, count + (i - 1) % count) for i in range(count)]
    return lax.ppermute(block, ("core", "dp"), up + down)


def across(block):
    count = lax.axis_size("dp")
    up = [(count + i, (i + 1) % count) for i in range(count)]
    down = [(i, count + (i - 1) % count) for i in range(count)]
    return lax.ppermute(block, ("core", "dp"), up + down)


def positions(member):
    count = member.shape[-1]
    row = lax.broadcasted_iota(jnp.int32, (count, count), 0)
    col = lax.broadcasted_iota(jnp.int32, (count, count), 1)
    before = (row < col).astype(jnp.bfloat16)
    return jnp.einsum(
        "...i,ij->...j", member.astype(jnp.bfloat16), before, preferred_element_type=jnp.float32
    ).astype(jnp.int32)


def with_ids(tokens, ids):
    tok_dev, width = tokens.shape
    picks = ids.shape[0]

    def body(tokens_ref, ids_ref, out_ref):
        out_ref[:tok_dev] = tokens_ref[...]
        found = ids_ref[...].astype(jnp.float32)
        tall = jnp.concatenate([found, jnp.zeros((picks, tok_dev), jnp.float32)], axis=0)
        wide = jnp.concatenate([tall, jnp.zeros((2 * picks, width - tok_dev), jnp.float32)], axis=1)
        out_ref[tok_dev:] = wide.astype(jnp.bfloat16)

    return pl.pallas_call(
        body,
        out_shape=jax.ShapeDtypeStruct((tok_dev + 2 * picks, width), jnp.bfloat16),
        compiler_params=pltpu.CompilerParams(vmem_limit_bytes=4 * 2**20),
        cost_estimate=pl.CostEstimate(flops=2 * tokens.size, bytes_accessed=4 * tokens.size, transcendentals=0),
    )(tokens, ids)


def chosen_rows(gathered, table, tok_dev, picks, chip_experts, capacity):
    sources, _, width = gathered.shape
    slots = chip_experts * capacity
    end = table.shape[0]

    def body(table_ref, gathered_ref, out_ref):
        row = lax.broadcasted_iota(jnp.int32, (tok_dev, tok_dev), 0)
        col = lax.broadcasted_iota(jnp.int32, (tok_dev, tok_dev), 1)
        before = (row < col).astype(jnp.bfloat16)
        lines = []
        for s in range(sources):
            ids = gathered_ref[s, tok_dev : tok_dev + picks, :tok_dev].astype(jnp.float32)
            for e in range(chip_experts):
                name = table_ref[end - 2] + lax.rem(table_ref[end - 1] + e, chip_experts)
                same = jnp.where(ids == name.astype(jnp.float32), 1.0, 0.0)
                lines.append(jnp.max(same, axis=0, keepdims=True))
        member = jnp.concatenate(lines, axis=0)
        spot = lax.dot_general(
            member.astype(jnp.bfloat16),
            before,
            (((1,), (0,)), ((), ())),
            preferred_element_type=jnp.float32,
        )
        spot = jnp.where(member > 0.5, spot, -1.0)
        slot = lax.broadcasted_iota(jnp.int32, (capacity, tok_dev), 0).astype(jnp.float32)
        for s in range(sources):
            picked = [
                jnp.where(spot[at : at + 1] == slot, 1.0, 0.0)
                for at in range(s * chip_experts, (s + 1) * chip_experts)
            ]
            found = lax.dot_general(
                jnp.concatenate(picked, axis=0).astype(jnp.bfloat16),
                gathered_ref[s, :tok_dev],
                (((1,), (0,)), ((), ())),
                preferred_element_type=jnp.float32,
            ).astype(jnp.bfloat16)
            for e in range(chip_experts):
                out_ref[e, s * capacity : (s + 1) * capacity] = found[
                    e * capacity : (e + 1) * capacity
                ]

    return pl.pallas_call(
        body,
        in_specs=[pl.BlockSpec(memory_space=pltpu.SMEM), pl.BlockSpec(memory_space=pltpu.VMEM)],
        out_specs=pl.BlockSpec(memory_space=pltpu.VMEM),
        out_shape=jax.ShapeDtypeStruct((chip_experts, sources * capacity, width), jnp.bfloat16),
        compiler_params=pltpu.CompilerParams(vmem_limit_bytes=16 * 2**20),
        cost_estimate=pl.CostEstimate(
            flops=2 * sources * slots * tok_dev * width,
            bytes_accessed=2 * gathered.size,
            transcendentals=0,
        ),
    )(table, gathered)


def weighted_sum(parts, steps, weights, table, kind, order, extra=(), finish=None, out=None):
    exp_dev = weights[0][0].shape[0]
    chip_experts = exp_dev * CORES
    n_kinds = len(weights)
    into = kind == "in"
    n_parts = len(parts)
    if into:
        hid, width = weights[0][0].shape[1], parts[0].shape[2]
        rows = parts[0].shape[1]
        sum_shape = (n_kinds * hid, rows)
        dims = (((1,), (1,)), ((), ()))
    else:
        hid, width = parts[0].shape[1], weights[0][0].shape[2]
        rows = parts[0].shape[2]
        sum_shape = (rows, width)
        dims = (((0,), (0,)), ((), ()))
    out_shape = out or jax.ShapeDtypeStruct((chip_experts, *sum_shape), jnp.float32)

    def body(table_ref, *refs):
        part_refs, rest = refs[:n_parts], refs[n_parts:]
        weight_refs, rest = rest[: 2 * n_kinds], rest[2 * n_kinds :]
        extra_refs, out_ref = rest[:-1], rest[-1]
        for e in range(chip_experts):
            side = order[e // exp_dev]
            sums = []
            for k in range(n_kinds):
                ref = weight_refs[2 * k + side]
                spot = (slice(k * hid, (k + 1) * hid),) if into else ()
                total = [x[(e, *spot)].astype(jnp.float32) for x in extra_refs]
                for part_ref, step in zip(part_refs, steps):
                    part = part_ref[e]
                    if into:
                        at = pl.ds(pl.multiple_of(table_ref[step] * width, width), width)
                        pair = (ref[e % exp_dev, :, at], part)
                    else:
                        at = pl.ds(pl.multiple_of(table_ref[step] * hid, hid), hid)
                        pair = (part, ref[e % exp_dev, at, :])
                    total.append(lax.dot_general(*pair, dims, preferred_element_type=jnp.float32))
                sums.append(sum(total[1:], total[0]))
            if finish is not None:
                finish(out_ref, e, *sums)
            elif into:
                for k, total in enumerate(sums):
                    out_ref[e, k * hid : (k + 1) * hid] = total.astype(out_ref.dtype)
            else:
                out_ref[e] = sums[0].astype(out_ref.dtype)

    whole = pl.BlockSpec(memory_space=pltpu.VMEM)
    operands = [*parts, *(w for pair in weights for w in pair), *extra]
    flops = 2 * chip_experts * n_parts * n_kinds * rows * hid * width
    moved = 2 * sum(x.size for x in operands)
    return pl.pallas_call(
        body,
        in_specs=[pl.BlockSpec(memory_space=pltpu.SMEM)] + [whole] * len(operands),
        out_specs=whole,
        out_shape=out_shape,
        compiler_params=pltpu.CompilerParams(vmem_limit_bytes=24 * 2**20),
        cost_estimate=pl.CostEstimate(flops=flops, bytes_accessed=moved, transcendentals=0),
    )(table, *operands)


def gather_sum(own, weights, owners, kind, finish, out):
    half = lax.axis_size("dp") // 2
    summed = lambda parts, steps, order, *rest: weighted_sum(
        parts, steps, weights, owners, kind, order, *rest
    )
    mine = [own]
    for _ in range(1, half + 1):
        mine.append(onward(mine[-1]))
    other = []
    for _ in range(1, half):
        other.append(onward(other[-1]) if other else across(own))
    early = summed(mine[: half - 1], range(half - 1), (0, 1))
    ahead = summed(other[:-1], range(1, half - 1), (1, 0))
    aside = summed(other[-1:], [half - 1], (1, 0), (ahead,))
    back = swap(aside)
    return summed(mine[half - 1 :], [half - 1, half], (0, 1), (early, back), finish, out)


def layer(tokens, expert_ids, gate_levels, gate_weight, up_weight, down_weight):
    tok_dev, _ = tokens.shape
    picks = expert_ids.shape[1]
    exp_dev = gate_weight.shape[0]
    hid = gate_weight.shape[2]
    n_z = lax.axis_size("z")
    chip_experts = exp_dev * CORES
    experts = chip_experts * n_z
    capacity = min(tok_dev, max(2, 2 * tok_dev * picks // experts))
    core = lax.axis_index("core")
    z = lax.axis_index("z")

    n_dp = lax.axis_size("dp")
    at = jnp.arange(n_dp + 2, dtype=jnp.int32)
    table = (lax.axis_index("dp") + jnp.where(core == 1, at, -at)) % n_dp
    table = jnp.where(at == n_dp, z * chip_experts, table)
    table = jnp.where(at == n_dp + 1, core * exp_dev, table)

    payload = with_ids(tokens, expert_ids.T)
    payload, table = lax.optimization_barrier((payload, table))
    gathered = lax.all_gather(payload, "z", axis=0)
    count = n_z * capacity
    rows = chosen_rows(gathered, table, tok_dev, picks, chip_experts, capacity)

    pairs = []
    for weights in (jnp.swapaxes(gate_weight, 1, 2), jnp.swapaxes(up_weight, 1, 2), down_weight):
        pairs.append((weights, swap(weights)))

    def gated(out_ref, e, gate_sum, up_sum):
        out_ref[e] = (gate_sum / (1.0 + jnp.exp(-gate_sum)) * up_sum).astype(jnp.bfloat16)

    hidden = gather_sum(
        rows,
        pairs[:2],
        table,
        "in",
        gated,
        jax.ShapeDtypeStruct((chip_experts, hid, count), jnp.bfloat16),
    )

    out_features = down_weight.shape[2]

    def returning(out_ref, e, total):
        out_ref[:, e] = total.astype(jnp.bfloat16).reshape(n_z, capacity, out_features)

    result = gather_sum(
        hidden,
        pairs[2:],
        table,
        "out",
        returning,
        jax.ShapeDtypeStruct((n_z, chip_experts, capacity, out_features), jnp.bfloat16),
    )
    returned = lax.all_to_all(result, "z", split_axis=0, concat_axis=0, tiled=True)
    slot_count = experts * capacity
    returned = returned.reshape(slot_count, out_features)

    own_ids = expert_ids.T
    every = jnp.arange(experts, dtype=jnp.int32)
    in_chip = every % chip_experts
    names = every - in_chip + (in_chip + core * exp_dev) % chip_experts
    named = own_ids[None, :, :] == names[:, None, None]
    own_spot = positions(jnp.any(named, axis=1))
    shares = gate_levels.astype(jnp.float32) / 256.0
    factor = jnp.sum(jnp.where(named, shares.T[None, :, :], 0.0), axis=1)
    weighting = jnp.where(
        own_spot[:, None, :] == jnp.arange(capacity, dtype=jnp.int32)[None, :, None],
        factor[:, None, :],
        0.0,
    ).astype(jnp.bfloat16)
    weighting = weighting.reshape(slot_count, tok_dev)
    combined = jnp.einsum("sj,sd->jd", weighting, returned, preferred_element_type=jnp.float32)
    return combined.astype(jnp.bfloat16)


def solution(mesh):
    groups, expert, dp = (mesh.shape[name] for name in ("groups", "expert", "dp"))
    split = Mesh(
        mesh.devices.reshape(groups, expert // CORES, CORES, dp), ("groups", "z", "core", "dp")
    )
    rows, held = ("groups", "z", "core"), ("z", "core")
    in_specs = (
        P(rows, "dp"),
        P(rows, None),
        P(rows, None),
        P(held, None, "dp"),
        P(held, None, "dp"),
        P(held, None, "dp"),
    )
    return jax.shard_map(
        layer, mesh=split, in_specs=in_specs, out_specs=P(rows, "dp"), check_vma=False
    )
```

```python
import jax
import jax.numpy as jnp
from jax import lax
from jax.experimental import pallas as pl
from jax.experimental.pallas import tpu as pltpu
from jax.sharding import Mesh, PartitionSpec as P


CORES = 2


def swap(block):
    return lax.ppermute(block, "core", [(0, 1), (1, 0)])


def onward(block):
    count = lax.axis_size("dp")
    up = [(i, (i + 1) % count) for i in range(count)]
    down = [(count + i, count + (i - 1) % count) for i in range(count)]
    return lax.ppermute(block, ("core", "dp"), up + down)


def across(block):
    count = lax.axis_size("dp")
    up = [(count + i, (i + 1) % count) for i in range(count)]
    down = [(i, count + (i - 1) % count) for i in range(count)]
    return lax.ppermute(block, ("core", "dp"), up + down)


def positions(member):
    count = member.shape[-1]
    row = lax.broadcasted_iota(jnp.int32, (count, count), 0)
    col = lax.broadcasted_iota(jnp.int32, (count, count), 1)
    before = (row < col).astype(jnp.bfloat16)
    return jnp.einsum(
        "...i,ij->...j", member.astype(jnp.bfloat16), before, preferred_element_type=jnp.float32
    ).astype(jnp.int32)


def with_ids(tokens, ids):
    tok_dev, width = tokens.shape
    picks = ids.shape[0]

    def body(tokens_ref, ids_ref, out_ref):
        out_ref[:tok_dev] = tokens_ref[...]
        found = ids_ref[...].astype(jnp.float32)
        tall = jnp.concatenate([found, jnp.zeros((picks, tok_dev), jnp.float32)], axis=0)
        wide = jnp.concatenate([tall, jnp.zeros((2 * picks, width - tok_dev), jnp.float32)], axis=1)
        out_ref[tok_dev:] = wide.astype(jnp.bfloat16)

    return pl.pallas_call(
        body,
        out_shape=jax.ShapeDtypeStruct((tok_dev + 2 * picks, width), jnp.bfloat16),
        compiler_params=pltpu.CompilerParams(vmem_limit_bytes=4 * 2**20),
        cost_estimate=pl.CostEstimate(flops=2 * tokens.size, bytes_accessed=4 * tokens.size, transcendentals=0),
    )(tokens, ids)


def chosen_rows(gathered, table, tok_dev, picks, chip_experts, capacity):
    sources, _, width = gathered.shape
    slots = chip_experts * capacity
    end = table.shape[0]

    def body(table_ref, gathered_ref, out_ref):
        row = lax.broadcasted_iota(jnp.int32, (tok_dev, tok_dev), 0)
        col = lax.broadcasted_iota(jnp.int32, (tok_dev, tok_dev), 1)
        before = (row < col).astype(jnp.bfloat16)
        lines = []
        for s in range(sources):
            ids = gathered_ref[s, tok_dev : tok_dev + picks, :tok_dev].astype(jnp.float32)
            for e in range(chip_experts):
                name = table_ref[end - 2] + lax.rem(table_ref[end - 1] + e, chip_experts)
                same = jnp.where(ids == name.astype(jnp.float32), 1.0, 0.0)
                lines.append(jnp.max(same, axis=0, keepdims=True))
        member = jnp.concatenate(lines, axis=0)
        spot = lax.dot_general(
            member.astype(jnp.bfloat16),
            before,
            (((1,), (0,)), ((), ())),
            preferred_element_type=jnp.float32,
        )
        spot = jnp.where(member > 0.5, spot, -1.0)
        slot = lax.broadcasted_iota(jnp.int32, (capacity, tok_dev), 0).astype(jnp.float32)
        for s in range(sources):
            picked = [
                jnp.where(spot[at : at + 1] == slot, 1.0, 0.0)
                for at in range(s * chip_experts, (s + 1) * chip_experts)
            ]
            found = lax.dot_general(
                jnp.concatenate(picked, axis=0).astype(jnp.bfloat16),
                gathered_ref[s, :tok_dev],
                (((1,), (0,)), ((), ())),
                preferred_element_type=jnp.float32,
            ).astype(jnp.bfloat16)
            for e in range(chip_experts):
                out_ref[e, s * capacity : (s + 1) * capacity] = found[
                    e * capacity : (e + 1) * capacity
                ]

    return pl.pallas_call(
        body,
        in_specs=[pl.BlockSpec(memory_space=pltpu.SMEM), pl.BlockSpec(memory_space=pltpu.VMEM)],
        out_specs=pl.BlockSpec(memory_space=pltpu.VMEM),
        out_shape=jax.ShapeDtypeStruct((chip_experts, sources * capacity, width), jnp.bfloat16),
        compiler_params=pltpu.CompilerParams(vmem_limit_bytes=16 * 2**20),
        cost_estimate=pl.CostEstimate(
            flops=2 * sources * slots * tok_dev * width,
            bytes_accessed=2 * gathered.size,
            transcendentals=0,
        ),
    )(table, gathered)


def weighted_sum(parts, steps, weights, table, kind, order, extra=(), finish=None, out=None):
    exp_dev = weights[0][0].shape[0]
    chip_experts = exp_dev * CORES
    n_kinds = len(weights)
    into = kind == "in"
    n_parts = len(parts)
    if into:
        hid, width = weights[0][0].shape[1], parts[0].shape[2]
        rows = parts[0].shape[1]
        sum_shape = (n_kinds * hid, rows)
        dims = (((1,), (1,)), ((), ()))
    else:
        hid, width = parts[0].shape[1], weights[0][0].shape[2]
        rows = parts[0].shape[2]
        sum_shape = (rows, width)
        dims = (((0,), (0,)), ((), ()))
    out_shape = out or jax.ShapeDtypeStruct((chip_experts, *sum_shape), jnp.float32)

    def body(table_ref, *refs):
        part_refs, rest = refs[:n_parts], refs[n_parts:]
        weight_refs, rest = rest[: 2 * n_kinds], rest[2 * n_kinds :]
        extra_refs, out_ref = rest[:-1], rest[-1]
        for e in range(chip_experts):
            side = order[e // exp_dev]
            sums = []
            for k in range(n_kinds):
                ref = weight_refs[2 * k + side]
                spot = (slice(k * hid, (k + 1) * hid),) if into else ()
                total = [x[(e, *spot)].astype(jnp.float32) for x in extra_refs]
                for part_ref, step in zip(part_refs, steps):
                    part = part_ref[e]
                    if into:
                        at = pl.ds(pl.multiple_of(table_ref[step] * width, width), width)
                        pair = (ref[e % exp_dev, :, at], part)
                    else:
                        at = pl.ds(pl.multiple_of(table_ref[step] * hid, hid), hid)
                        pair = (part, ref[e % exp_dev, at, :])
                    total.append(lax.dot_general(*pair, dims, preferred_element_type=jnp.float32))
                sums.append(sum(total[1:], total[0]))
            if finish is not None:
                finish(out_ref, e, *sums)
            elif into:
                for k, total in enumerate(sums):
                    out_ref[e, k * hid : (k + 1) * hid] = total.astype(out_ref.dtype)
            else:
                out_ref[e] = sums[0].astype(out_ref.dtype)

    whole = pl.BlockSpec(memory_space=pltpu.VMEM)
    operands = [*parts, *(w for pair in weights for w in pair), *extra]
    flops = 2 * chip_experts * n_parts * n_kinds * rows * hid * width
    moved = 2 * sum(x.size for x in operands)
    return pl.pallas_call(
        body,
        in_specs=[pl.BlockSpec(memory_space=pltpu.SMEM)] + [whole] * len(operands),
        out_specs=whole,
        out_shape=out_shape,
        compiler_params=pltpu.CompilerParams(vmem_limit_bytes=24 * 2**20),
        cost_estimate=pl.CostEstimate(flops=flops, bytes_accessed=moved, transcendentals=0),
    )(table, *operands)


def gather_sum(own, weights, owners, kind, direct, finish, out):
    half = lax.axis_size("dp") // 2
    summed = lambda parts, steps, order, *rest: weighted_sum(
        parts, steps, weights, owners, kind, order, *rest
    )
    mine = [own]
    for _ in range(1, half + 1):
        mine.append(onward(mine[-1]))
    if direct:
        other = [across(own)]
    else:
        paired = swap(own)
        other = [onward(paired)]
    for _ in range(2, half):
        other.append(onward(other[-1]))
    early = summed(mine[: half - 1], range(half - 1), (0, 1))
    ahead = summed(other[:-1], range(1, half - 1), (1, 0))
    aside = summed(other[-1:], [half - 1], (1, 0), (ahead,))
    back = swap(aside)
    return summed(mine[half - 1 :], [half - 1, half], (0, 1), (early, back), finish, out)


def layer(tokens, expert_ids, gate_levels, gate_weight, up_weight, down_weight):
    tok_dev, _ = tokens.shape
    picks = expert_ids.shape[1]
    exp_dev = gate_weight.shape[0]
    hid = gate_weight.shape[2]
    n_z = lax.axis_size("z")
    chip_experts = exp_dev * CORES
    experts = chip_experts * n_z
    capacity = min(tok_dev, max(2, 2 * tok_dev * picks // experts))
    core = lax.axis_index("core")
    z = lax.axis_index("z")

    n_dp = lax.axis_size("dp")
    at = jnp.arange(n_dp + 2, dtype=jnp.int32)
    table = (lax.axis_index("dp") + jnp.where(core == 1, at, -at)) % n_dp
    table = jnp.where(at == n_dp, z * chip_experts, table)
    table = jnp.where(at == n_dp + 1, core * exp_dev, table)

    payload = with_ids(tokens, expert_ids.T)
    payload, table = lax.optimization_barrier((payload, table))
    gathered = lax.all_gather(payload, "z", axis=0)
    count = n_z * capacity
    rows = chosen_rows(gathered, table, tok_dev, picks, chip_experts, capacity)

    pairs = []
    for weights in (jnp.swapaxes(gate_weight, 1, 2), jnp.swapaxes(up_weight, 1, 2), down_weight):
        pairs.append((weights, swap(weights)))

    def gated(out_ref, e, gate_sum, up_sum):
        out_ref[e] = (gate_sum / (1.0 + jnp.exp(-gate_sum)) * up_sum).astype(jnp.bfloat16)

    hidden = gather_sum(
        rows,
        pairs[:2],
        table,
        "in",
        False,
        gated,
        jax.ShapeDtypeStruct((chip_experts, hid, count), jnp.bfloat16),
    )

    out_features = down_weight.shape[2]

    def returning(out_ref, e, total):
        out_ref[:, e] = total.astype(jnp.bfloat16).reshape(n_z, capacity, out_features)

    result = gather_sum(
        hidden,
        pairs[2:],
        table,
        "out",
        True,
        returning,
        jax.ShapeDtypeStruct((n_z, chip_experts, capacity, out_features), jnp.bfloat16),
    )
    returned = lax.all_to_all(result, "z", split_axis=0, concat_axis=0, tiled=True)
    slot_count = experts * capacity
    returned = returned.reshape(slot_count, out_features)

    own_ids = expert_ids.T
    every = jnp.arange(experts, dtype=jnp.int32)
    in_chip = every % chip_experts
    names = every - in_chip + (in_chip + core * exp_dev) % chip_experts
    named = own_ids[None, :, :] == names[:, None, None]
    own_spot = positions(jnp.any(named, axis=1))
    shares = gate_levels.astype(jnp.float32) / 256.0
    factor = jnp.sum(jnp.where(named, shares.T[None, :, :], 0.0), axis=1)
    weighting = jnp.where(
        own_spot[:, None, :] == jnp.arange(capacity, dtype=jnp.int32)[None, :, None],
        factor[:, None, :],
        0.0,
    ).astype(jnp.bfloat16)
    weighting = weighting.reshape(slot_count, tok_dev)
    combined = jnp.einsum("sj,sd->jd", weighting, returned, preferred_element_type=jnp.float32)
    return combined.astype(jnp.bfloat16)


def solution(mesh):
    groups, expert, dp = (mesh.shape[name] for name in ("groups", "expert", "dp"))
    split = Mesh(
        mesh.devices.reshape(groups, expert // CORES, CORES, dp), ("groups", "z", "core", "dp")
    )
    rows, held = ("groups", "z", "core"), ("z", "core")
    in_specs = (
        P(rows, "dp"),
        P(rows, None),
        P(rows, None),
        P(held, None, "dp"),
        P(held, None, "dp"),
        P(held, None, "dp"),
    )
    return jax.shard_map(
        layer, mesh=split, in_specs=in_specs, out_specs=P(rows, "dp"), check_vma=False
    )
```

```python
import jax
import jax.numpy as jnp
from jax import lax
from jax.experimental import pallas as pl
from jax.experimental.pallas import tpu as pltpu
from jax.sharding import Mesh, PartitionSpec as P


CORES = 2
Z = ("far", "near")


def swap(block):
    return lax.ppermute(block, "core", [(0, 1), (1, 0)])


def onward(block):
    count = lax.axis_size("dp")
    up = [(i, (i + 1) % count) for i in range(count)]
    down = [(count + i, count + (i - 1) % count) for i in range(count)]
    return lax.ppermute(block, ("core", "dp"), up + down)


def across(block):
    count = lax.axis_size("dp")
    up = [(count + i, (i + 1) % count) for i in range(count)]
    down = [(i, count + (i - 1) % count) for i in range(count)]
    return lax.ppermute(block, ("core", "dp"), up + down)


def positions(member):
    count = member.shape[-1]
    row = lax.broadcasted_iota(jnp.int32, (count, count), 0)
    col = lax.broadcasted_iota(jnp.int32, (count, count), 1)
    before = (row < col).astype(jnp.bfloat16)
    return jnp.einsum(
        "...i,ij->...j", member.astype(jnp.bfloat16), before, preferred_element_type=jnp.float32
    ).astype(jnp.int32)


def with_ids(tokens, ids):
    tok_dev, width = tokens.shape
    picks = ids.shape[0]

    def body(tokens_ref, ids_ref, out_ref):
        out_ref[:tok_dev] = tokens_ref[...]
        found = ids_ref[...].astype(jnp.float32)
        tall = jnp.concatenate([found, jnp.zeros((picks, tok_dev), jnp.float32)], axis=0)
        wide = jnp.concatenate([tall, jnp.zeros((2 * picks, width - tok_dev), jnp.float32)], axis=1)
        out_ref[tok_dev:] = wide.astype(jnp.bfloat16)

    return pl.pallas_call(
        body,
        out_shape=jax.ShapeDtypeStruct((tok_dev + 2 * picks, width), jnp.bfloat16),
        compiler_params=pltpu.CompilerParams(vmem_limit_bytes=4 * 2**20),
        cost_estimate=pl.CostEstimate(flops=2 * tokens.size, bytes_accessed=4 * tokens.size, transcendentals=0),
    )(tokens, ids)


def chosen_rows(gathered, table, tok_dev, picks, chip_experts, capacity):
    near, far, _, width = gathered.shape
    sources = near * far
    slots = chip_experts * capacity
    end = table.shape[0]

    def body(table_ref, gathered_ref, out_ref):
        row = lax.broadcasted_iota(jnp.int32, (tok_dev, tok_dev), 0)
        col = lax.broadcasted_iota(jnp.int32, (tok_dev, tok_dev), 1)
        before = (row < col).astype(jnp.bfloat16)
        lines = []
        for s in range(sources):
            ids = gathered_ref[s % near, s // near, tok_dev : tok_dev + picks, :tok_dev].astype(jnp.float32)
            for e in range(chip_experts):
                name = table_ref[end - 2] + lax.rem(table_ref[end - 1] + e, chip_experts)
                same = jnp.where(ids == name.astype(jnp.float32), 1.0, 0.0)
                lines.append(jnp.max(same, axis=0, keepdims=True))
        member = jnp.concatenate(lines, axis=0)
        spot = lax.dot_general(
            member.astype(jnp.bfloat16),
            before,
            (((1,), (0,)), ((), ())),
            preferred_element_type=jnp.float32,
        )
        spot = jnp.where(member > 0.5, spot, -1.0)
        slot = lax.broadcasted_iota(jnp.int32, (capacity, tok_dev), 0).astype(jnp.float32)
        for s in range(sources):
            picked = [
                jnp.where(spot[at : at + 1] == slot, 1.0, 0.0)
                for at in range(s * chip_experts, (s + 1) * chip_experts)
            ]
            found = lax.dot_general(
                jnp.concatenate(picked, axis=0).astype(jnp.bfloat16),
                gathered_ref[s % near, s // near, :tok_dev],
                (((1,), (0,)), ((), ())),
                preferred_element_type=jnp.float32,
            ).astype(jnp.bfloat16)
            for e in range(chip_experts):
                out_ref[e, s * capacity : (s + 1) * capacity] = found[
                    e * capacity : (e + 1) * capacity
                ]

    return pl.pallas_call(
        body,
        in_specs=[pl.BlockSpec(memory_space=pltpu.SMEM), pl.BlockSpec(memory_space=pltpu.VMEM)],
        out_specs=pl.BlockSpec(memory_space=pltpu.VMEM),
        out_shape=jax.ShapeDtypeStruct((chip_experts, sources * capacity, width), jnp.bfloat16),
        compiler_params=pltpu.CompilerParams(vmem_limit_bytes=16 * 2**20),
        cost_estimate=pl.CostEstimate(
            flops=2 * sources * slots * tok_dev * width,
            bytes_accessed=2 * gathered.size,
            transcendentals=0,
        ),
    )(table, gathered)


def weighted_sum(parts, steps, weights, table, kind, order, extra=(), finish=None, out=None):
    exp_dev = weights[0][0].shape[0]
    chip_experts = exp_dev * CORES
    n_kinds = len(weights)
    into = kind == "in"
    n_parts = len(parts)
    if into:
        hid, width = weights[0][0].shape[1], parts[0].shape[2]
        rows = parts[0].shape[1]
        sum_shape = (n_kinds * hid, rows)
        dims = (((1,), (1,)), ((), ()))
    else:
        hid, width = parts[0].shape[1], weights[0][0].shape[2]
        rows = parts[0].shape[2]
        sum_shape = (rows, width)
        dims = (((0,), (0,)), ((), ()))
    out_shape = out or jax.ShapeDtypeStruct((chip_experts, *sum_shape), jnp.float32)

    def body(table_ref, *refs):
        part_refs, rest = refs[:n_parts], refs[n_parts:]
        weight_refs, rest = rest[: 2 * n_kinds], rest[2 * n_kinds :]
        extra_refs, out_ref = rest[:-1], rest[-1]
        for e in range(chip_experts):
            side = order[e // exp_dev]
            sums = []
            for k in range(n_kinds):
                ref = weight_refs[2 * k + side]
                spot = (slice(k * hid, (k + 1) * hid),) if into else ()
                total = [x[(e, *spot)].astype(jnp.float32) for x in extra_refs]
                for part_ref, step in zip(part_refs, steps):
                    part = part_ref[e]
                    if into:
                        at = pl.ds(pl.multiple_of(table_ref[step] * width, width), width)
                        pair = (ref[e % exp_dev, :, at], part)
                    else:
                        at = pl.ds(pl.multiple_of(table_ref[step] * hid, hid), hid)
                        pair = (part, ref[e % exp_dev, at, :])
                    total.append(lax.dot_general(*pair, dims, preferred_element_type=jnp.float32))
                sums.append(sum(total[1:], total[0]))
            if finish is not None:
                finish(out_ref, e, *sums)
            elif into:
                for k, total in enumerate(sums):
                    out_ref[e, k * hid : (k + 1) * hid] = total.astype(out_ref.dtype)
            else:
                out_ref[e] = sums[0].astype(out_ref.dtype)

    whole = pl.BlockSpec(memory_space=pltpu.VMEM)
    operands = [*parts, *(w for pair in weights for w in pair), *extra]
    flops = 2 * chip_experts * n_parts * n_kinds * rows * hid * width
    moved = 2 * sum(x.size for x in operands)
    return pl.pallas_call(
        body,
        in_specs=[pl.BlockSpec(memory_space=pltpu.SMEM)] + [whole] * len(operands),
        out_specs=whole,
        out_shape=out_shape,
        compiler_params=pltpu.CompilerParams(vmem_limit_bytes=24 * 2**20),
        cost_estimate=pl.CostEstimate(flops=flops, bytes_accessed=moved, transcendentals=0),
    )(table, *operands)


def gather_sum(own, weights, owners, kind, direct, finish, out):
    half = lax.axis_size("dp") // 2
    summed = lambda parts, steps, order, *rest: weighted_sum(
        parts, steps, weights, owners, kind, order, *rest
    )
    mine = [own]
    for _ in range(1, half + 1):
        mine.append(onward(mine[-1]))
    if direct:
        other = [across(own)]
    else:
        paired = swap(own)
        other = [onward(paired)]
    for _ in range(2, half):
        other.append(onward(other[-1]))
    early = summed(mine[: half - 1], range(half - 1), (0, 1))
    ahead = summed(other[:-1], range(1, half - 1), (1, 0))
    aside = summed(other[-1:], [half - 1], (1, 0), (ahead,))
    back = swap(aside)
    return summed(mine[half - 1 :], [half - 1, half], (0, 1), (early, back), finish, out)


def layer(tokens, expert_ids, gate_levels, gate_weight, up_weight, down_weight):
    tok_dev, _ = tokens.shape
    picks = expert_ids.shape[1]
    exp_dev = gate_weight.shape[0]
    hid = gate_weight.shape[2]
    n_z = lax.axis_size(Z)
    chip_experts = exp_dev * CORES
    experts = chip_experts * n_z
    capacity = min(tok_dev, max(2, 2 * tok_dev * picks // experts))
    core = lax.axis_index("core")
    z = lax.axis_index(Z)

    n_dp = lax.axis_size("dp")
    at = jnp.arange(n_dp + 2, dtype=jnp.int32)
    table = (lax.axis_index("dp") + jnp.where(core == 1, at, -at)) % n_dp
    table = jnp.where(at == n_dp, z * chip_experts, table)
    table = jnp.where(at == n_dp + 1, core * exp_dev, table)

    payload = with_ids(tokens, expert_ids.T)
    payload, table = lax.optimization_barrier((payload, table))
    gathered = lax.all_gather(payload, "far", axis=0)
    gathered = lax.all_gather(gathered, "near", axis=0)
    count = n_z * capacity
    rows = chosen_rows(gathered, table, tok_dev, picks, chip_experts, capacity)

    pairs = []
    for weights in (jnp.swapaxes(gate_weight, 1, 2), jnp.swapaxes(up_weight, 1, 2), down_weight):
        pairs.append((weights, swap(weights)))

    def gated(out_ref, e, gate_sum, up_sum):
        out_ref[e] = (gate_sum / (1.0 + jnp.exp(-gate_sum)) * up_sum).astype(jnp.bfloat16)

    hidden = gather_sum(
        rows,
        pairs[:2],
        table,
        "in",
        False,
        gated,
        jax.ShapeDtypeStruct((chip_experts, hid, count), jnp.bfloat16),
    )

    out_features = down_weight.shape[2]

    def returning(out_ref, e, total):
        out_ref[:, e] = total.astype(jnp.bfloat16).reshape(n_z, capacity, out_features)

    result = gather_sum(
        hidden,
        pairs[2:],
        table,
        "out",
        True,
        returning,
        jax.ShapeDtypeStruct((n_z, chip_experts, capacity, out_features), jnp.bfloat16),
    )
    returned = lax.all_to_all(result, Z, split_axis=0, concat_axis=0, tiled=True)
    slot_count = experts * capacity
    returned = returned.reshape(slot_count, out_features)

    own_ids = expert_ids.T
    every = jnp.arange(experts, dtype=jnp.int32)
    in_chip = every % chip_experts
    names = every - in_chip + (in_chip + core * exp_dev) % chip_experts
    named = own_ids[None, :, :] == names[:, None, None]
    own_spot = positions(jnp.any(named, axis=1))
    shares = gate_levels.astype(jnp.float32) / 256.0
    factor = jnp.sum(jnp.where(named, shares.T[None, :, :], 0.0), axis=1)
    weighting = jnp.where(
        own_spot[:, None, :] == jnp.arange(capacity, dtype=jnp.int32)[None, :, None],
        factor[:, None, :],
        0.0,
    ).astype(jnp.bfloat16)
    weighting = weighting.reshape(slot_count, tok_dev)
    combined = jnp.einsum("sj,sd->jd", weighting, returned, preferred_element_type=jnp.float32)
    return combined.astype(jnp.bfloat16)


def solution(mesh):
    groups, expert, dp = (mesh.shape[name] for name in ("groups", "expert", "dp"))
    chips = expert // CORES
    near = 4 if chips % 4 == 0 else 1
    split = Mesh(
        mesh.devices.reshape(groups, chips // near, near, CORES, dp),
        ("groups", *Z, "core", "dp"),
    )
    rows, held = ("groups", *Z, "core"), (*Z, "core")
    in_specs = (
        P(rows, "dp"),
        P(rows, None),
        P(rows, None),
        P(held, None, "dp"),
        P(held, None, "dp"),
        P(held, None, "dp"),
    )
    return jax.shard_map(
        layer, mesh=split, in_specs=in_specs, out_specs=P(rows, "dp"), check_vma=False
    )
```

```python
import jax
import jax.numpy as jnp
from jax import lax
from jax.experimental import pallas as pl
from jax.experimental.pallas import tpu as pltpu
from jax.sharding import Mesh, PartitionSpec as P


CORES = 2


def swap(block):
    return lax.ppermute(block, "core", [(0, 1), (1, 0)])


def onward(block):
    count = lax.axis_size("dp")
    up = [(i, (i + 1) % count) for i in range(count)]
    down = [(count + i, count + (i - 1) % count) for i in range(count)]
    return lax.ppermute(block, ("core", "dp"), up + down)


def across(block):
    count = lax.axis_size("dp")
    up = [(count + i, (i + 1) % count) for i in range(count)]
    down = [(i, count + (i - 1) % count) for i in range(count)]
    return lax.ppermute(block, ("core", "dp"), up + down)


def positions(member):
    count = member.shape[-1]
    row = lax.broadcasted_iota(jnp.int32, (count, count), 0)
    col = lax.broadcasted_iota(jnp.int32, (count, count), 1)
    before = (row < col).astype(jnp.bfloat16)
    return jnp.einsum(
        "...i,ij->...j", member.astype(jnp.bfloat16), before, preferred_element_type=jnp.float32
    ).astype(jnp.int32)


def with_ids(tokens, ids):
    tok_dev, width = tokens.shape
    picks = ids.shape[0]

    def body(tokens_ref, ids_ref, out_ref, held_ref, sems):
        ids_copy = pltpu.make_async_copy(ids_ref, held_ref, sems.at[0])
        tokens_copy = pltpu.make_async_copy(tokens_ref, out_ref.at[:tok_dev], sems.at[1])
        ids_copy.start()
        tokens_copy.start()
        ids_copy.wait()
        found = held_ref[...].astype(jnp.float32)
        tall = jnp.concatenate([found, jnp.zeros((picks, tok_dev), jnp.float32)], axis=0)
        wide = jnp.concatenate([tall, jnp.zeros((2 * picks, width - tok_dev), jnp.float32)], axis=1)
        out_ref[tok_dev:] = wide.astype(jnp.bfloat16)
        tokens_copy.wait()

    return pl.pallas_call(
        body,
        in_specs=[pl.BlockSpec(memory_space=pl.ANY)] * 2,
        out_specs=pl.BlockSpec(memory_space=pltpu.VMEM),
        out_shape=jax.ShapeDtypeStruct((tok_dev + 2 * picks, width), jnp.bfloat16),
        scratch_shapes=[
            pltpu.VMEM((picks, tok_dev), jnp.int32),
            pltpu.SemaphoreType.DMA((2,)),
        ],
        cost_estimate=pl.CostEstimate(
            flops=2 * tokens.size, bytes_accessed=4 * tokens.size, transcendentals=0
        ),
    )(tokens, ids)


def chosen_rows(gathered, table, tok_dev, picks, chip_experts, capacity):
    sources, _, width = gathered.shape
    slots = chip_experts * capacity
    end = table.shape[0]

    def body(table_ref, gathered_ref, out_ref):
        row = lax.broadcasted_iota(jnp.int32, (tok_dev, tok_dev), 0)
        col = lax.broadcasted_iota(jnp.int32, (tok_dev, tok_dev), 1)
        before = (row < col).astype(jnp.bfloat16)
        lines = []
        for s in range(sources):
            ids = gathered_ref[s, tok_dev : tok_dev + picks, :tok_dev].astype(jnp.float32)
            for e in range(chip_experts):
                name = table_ref[end - 2] + lax.rem(table_ref[end - 1] + e, chip_experts)
                same = jnp.where(ids == name.astype(jnp.float32), 1.0, 0.0)
                lines.append(jnp.max(same, axis=0, keepdims=True))
        member = jnp.concatenate(lines, axis=0)
        spot = lax.dot_general(
            member.astype(jnp.bfloat16),
            before,
            (((1,), (0,)), ((), ())),
            preferred_element_type=jnp.float32,
        )
        spot = jnp.where(member > 0.5, spot, -1.0)
        slot = lax.broadcasted_iota(jnp.int32, (capacity, tok_dev), 0).astype(jnp.float32)
        for s in range(sources):
            picked = [
                jnp.where(spot[at : at + 1] == slot, 1.0, 0.0)
                for at in range(s * chip_experts, (s + 1) * chip_experts)
            ]
            found = lax.dot_general(
                jnp.concatenate(picked, axis=0).astype(jnp.bfloat16),
                gathered_ref[s, :tok_dev],
                (((1,), (0,)), ((), ())),
                preferred_element_type=jnp.float32,
            ).astype(jnp.bfloat16)
            for e in range(chip_experts):
                out_ref[e, s * capacity : (s + 1) * capacity] = found[
                    e * capacity : (e + 1) * capacity
                ]

    return pl.pallas_call(
        body,
        in_specs=[pl.BlockSpec(memory_space=pltpu.SMEM), pl.BlockSpec(memory_space=pltpu.VMEM)],
        out_specs=pl.BlockSpec(memory_space=pltpu.VMEM),
        out_shape=jax.ShapeDtypeStruct((chip_experts, sources * capacity, width), jnp.bfloat16),
        compiler_params=pltpu.CompilerParams(vmem_limit_bytes=16 * 2**20),
        cost_estimate=pl.CostEstimate(
            flops=2 * sources * slots * tok_dev * width,
            bytes_accessed=2 * gathered.size,
            transcendentals=0,
        ),
    )(table, gathered)


def weighted_sum(parts, steps, weights, table, kind, order, extra=(), finish=None, out=None):
    exp_dev = weights[0][0].shape[0]
    chip_experts = exp_dev * CORES
    n_kinds = len(weights)
    into = kind == "in"
    n_parts = len(parts)
    if into:
        hid, width = weights[0][0].shape[1], parts[0].shape[2]
        rows = parts[0].shape[1]
        sum_shape = (n_kinds * hid, rows)
        dims = (((1,), (1,)), ((), ()))
    else:
        hid, width = parts[0].shape[1], weights[0][0].shape[2]
        rows = parts[0].shape[2]
        sum_shape = (rows, width)
        dims = (((0,), (0,)), ((), ()))
    out_shape = out or jax.ShapeDtypeStruct((chip_experts, *sum_shape), jnp.float32)

    def body(table_ref, *refs):
        part_refs, rest = refs[:n_parts], refs[n_parts:]
        weight_refs, rest = rest[: 2 * n_kinds], rest[2 * n_kinds :]
        extra_refs, out_ref = rest[:-1], rest[-1]
        for e in range(chip_experts):
            side = order[e // exp_dev]
            sums = []
            for k in range(n_kinds):
                ref = weight_refs[2 * k + side]
                spot = (slice(k * hid, (k + 1) * hid),) if into else ()
                total = [x[(e, *spot)].astype(jnp.float32) for x in extra_refs]
                for part_ref, step in zip(part_refs, steps):
                    part = part_ref[e]
                    if into:
                        at = pl.ds(pl.multiple_of(table_ref[step] * width, width), width)
                        pair = (ref[e % exp_dev, :, at], part)
                    else:
                        at = pl.ds(pl.multiple_of(table_ref[step] * hid, hid), hid)
                        pair = (part, ref[e % exp_dev, at, :])
                    total.append(lax.dot_general(*pair, dims, preferred_element_type=jnp.float32))
                sums.append(sum(total[1:], total[0]))
            if finish is not None:
                finish(out_ref, e, *sums)
            elif into:
                for k, total in enumerate(sums):
                    out_ref[e, k * hid : (k + 1) * hid] = total.astype(out_ref.dtype)
            else:
                out_ref[e] = sums[0].astype(out_ref.dtype)

    whole = pl.BlockSpec(memory_space=pltpu.VMEM)
    operands = [*parts, *(w for pair in weights for w in pair), *extra]
    flops = 2 * chip_experts * n_parts * n_kinds * rows * hid * width
    moved = 2 * sum(x.size for x in operands)
    return pl.pallas_call(
        body,
        in_specs=[pl.BlockSpec(memory_space=pltpu.SMEM)] + [whole] * len(operands),
        out_specs=whole,
        out_shape=out_shape,
        compiler_params=pltpu.CompilerParams(vmem_limit_bytes=24 * 2**20),
        cost_estimate=pl.CostEstimate(flops=flops, bytes_accessed=moved, transcendentals=0),
    )(table, *operands)


def gather_sum(own, weights, owners, kind, direct, finish, out):
    half = lax.axis_size("dp") // 2
    summed = lambda parts, steps, order, *rest: weighted_sum(
        parts, steps, weights, owners, kind, order, *rest
    )
    mine = [own]
    for _ in range(1, half + 1):
        mine.append(onward(mine[-1]))
    if direct:
        other = [across(own)]
    else:
        paired = swap(own)
        other = [onward(paired)]
    for _ in range(2, half):
        other.append(onward(other[-1]))
    early = summed(mine[: half - 1], range(half - 1), (0, 1))
    ahead = summed(other[:-1], range(1, half - 1), (1, 0))
    aside = summed(other[-1:], [half - 1], (1, 0), (ahead,))
    back = swap(aside)
    return summed(mine[half - 1 :], [half - 1, half], (0, 1), (early, back), finish, out)


def layer(tokens, expert_ids, gate_levels, gate_weight, up_weight, down_weight):
    tok_dev, _ = tokens.shape
    picks = expert_ids.shape[1]
    exp_dev = gate_weight.shape[0]
    hid = gate_weight.shape[2]
    n_z = lax.axis_size("z")
    chip_experts = exp_dev * CORES
    experts = chip_experts * n_z
    capacity = min(tok_dev, max(2, 2 * tok_dev * picks // experts))
    core = lax.axis_index("core")
    z = lax.axis_index("z")

    n_dp = lax.axis_size("dp")
    at = jnp.arange(n_dp + 2, dtype=jnp.int32)
    table = (lax.axis_index("dp") + jnp.where(core == 1, at, -at)) % n_dp
    table = jnp.where(at == n_dp, z * chip_experts, table)
    table = jnp.where(at == n_dp + 1, core * exp_dev, table)

    payload = with_ids(tokens, expert_ids.T)
    payload, table = lax.optimization_barrier((payload, table))
    gathered = lax.all_gather(payload, "z", axis=0)
    count = n_z * capacity
    rows = chosen_rows(gathered, table, tok_dev, picks, chip_experts, capacity)

    pairs = []
    for weights in (jnp.swapaxes(gate_weight, 1, 2), jnp.swapaxes(up_weight, 1, 2), down_weight):
        pairs.append((weights, swap(weights)))

    def gated(out_ref, e, gate_sum, up_sum):
        out_ref[e] = (gate_sum / (1.0 + jnp.exp(-gate_sum)) * up_sum).astype(jnp.bfloat16)

    hidden = gather_sum(
        rows,
        pairs[:2],
        table,
        "in",
        False,
        gated,
        jax.ShapeDtypeStruct((chip_experts, hid, count), jnp.bfloat16),
    )

    out_features = down_weight.shape[2]

    def returning(out_ref, e, total):
        out_ref[:, e] = total.astype(jnp.bfloat16).reshape(n_z, capacity, out_features)

    result = gather_sum(
        hidden,
        pairs[2:],
        table,
        "out",
        True,
        returning,
        jax.ShapeDtypeStruct((n_z, chip_experts, capacity, out_features), jnp.bfloat16),
    )
    returned = lax.all_to_all(result, "z", split_axis=0, concat_axis=0, tiled=True)
    slot_count = experts * capacity
    returned = returned.reshape(slot_count, out_features)

    own_ids = expert_ids.T
    every = jnp.arange(experts, dtype=jnp.int32)
    in_chip = every % chip_experts
    names = every - in_chip + (in_chip + core * exp_dev) % chip_experts
    named = own_ids[None, :, :] == names[:, None, None]
    own_spot = positions(jnp.any(named, axis=1))
    shares = gate_levels.astype(jnp.float32) / 256.0
    factor = jnp.sum(jnp.where(named, shares.T[None, :, :], 0.0), axis=1)
    weighting = jnp.where(
        own_spot[:, None, :] == jnp.arange(capacity, dtype=jnp.int32)[None, :, None],
        factor[:, None, :],
        0.0,
    ).astype(jnp.bfloat16)
    weighting = weighting.reshape(slot_count, tok_dev)
    combined = jnp.einsum("sj,sd->jd", weighting, returned, preferred_element_type=jnp.float32)
    return combined.astype(jnp.bfloat16)


def solution(mesh):
    groups, expert, dp = (mesh.shape[name] for name in ("groups", "expert", "dp"))
    split = Mesh(
        mesh.devices.reshape(groups, expert // CORES, CORES, dp), ("groups", "z", "core", "dp")
    )
    rows, held = ("groups", "z", "core"), ("z", "core")
    in_specs = (
        P(rows, "dp"),
        P(rows, None),
        P(rows, None),
        P(held, None, "dp"),
        P(held, None, "dp"),
        P(held, None, "dp"),
    )
    return jax.shard_map(
        layer, mesh=split, in_specs=in_specs, out_specs=P(rows, "dp"), check_vma=False
    )
```
